64 devices in a mesh: dp: 4 (over x, y), ctx: 16 (over z, core).
Axes of the slice: x: 2, y: 2, z: 8, core: 2. Of those that a mesh axis runs over, the one named last changes fastest.
The devices are a block of a 4x4x8 slice.
Arguments:
- queries: bfloat16 [32, 4096, 4, 128], P('dp', 'ctx'), parts along dimension 0
- keys: bfloat16 [32, 4096, 1, 128], P('dp', 'ctx'), parts along dimension 0
- values: bfloat16 [32, 4096, 1, 128], P('dp', 'ctx'), parts along dimension 0
- grad_out: bfloat16 [32, 4096, 4, 128], P('dp', 'ctx'), parts along dimension 0
Outputs:
- output 1: bfloat16 [32, 4096, 4, 128], P('dp', 'ctx'), parts along dimension 0
- output 2: bfloat16 [32, 4096, 4, 128], P('dp', 'ctx'), parts along dimension 0
- output 3: bfloat16 [32, 4096, 1, 128], P('dp', 'ctx'), parts along dimension 0
- output 4: bfloat16 [32, 4096, 1, 128], P('dp', 'ctx'), parts along dimension 0
There are 4 independent parts. The reference program is written for one: setup_inputs(seed, part) draws one part's arguments, and reference() takes and returns one part's arrays. A program takes and returns all parts, laid end to end along the dimension named above; each array names one.
All inputs are finite; a program needn't handle non-finite values.
Results may differ from the reference program's by a relative error of at most 0.00597021.
Values are sent between devices in bfloat16 or wider.
A program may use at most 768 MiB of HBM per device.

```python
import jax
import jax.numpy as jnp
from jax import lax

BATCH = 8
SEQ = 4096
HQ = 4
HEAD_DIM = 128
BLOCK = 256
NEG_BIG = -1e30


def setup_inputs(seed: int = 0, part: int = 0) -> dict:
    part_key = jax.random.fold_in(jax.random.key(seed), part)
    key_q, key_k, key_v, key_do = jax.random.split(part_key, 4)
    q_shape = (BATCH, SEQ, HQ, HEAD_DIM)
    kv_shape = (BATCH, SEQ, 1, HEAD_DIM)
    queries = 1.5 * jax.random.normal(key_q, q_shape, jnp.float32)
    keys = jax.random.normal(key_k, kv_shape, jnp.float32)
    values = jax.random.normal(key_v, kv_shape, jnp.float32)
    grad_out = jax.random.normal(key_do, q_shape, jnp.float32)
    return {"queries": queries.astype(jnp.bfloat16), "keys": keys.astype(jnp.bfloat16), "values": values.astype(jnp.bfloat16), "grad_out": grad_out.astype(jnp.bfloat16)}


def reference(queries, keys, values, grad_out):
    n_kv = keys.shape[2]
    n_grp = HQ // n_kv
    n_blocks = SEQ // BLOCK
    scale = HEAD_DIM ** -0.5
    q_lead = jnp.moveaxis(queries.reshape(BATCH, n_blocks, BLOCK, n_kv, n_grp, HEAD_DIM), 1, 0)
    do_lead = jnp.moveaxis(grad_out.reshape(BATCH, n_blocks, BLOCK, n_kv, n_grp, HEAD_DIM), 1, 0)
    k_blocks = keys.reshape(BATCH, n_blocks, BLOCK, n_kv, HEAD_DIM)
    v_blocks = values.reshape(BATCH, n_blocks, BLOCK, n_kv, HEAD_DIM)
    blk_ids = jnp.arange(n_blocks)
    stat_shape = (BATCH, n_kv, n_grp, BLOCK)

    def block_scores(q_blk, k_blk, blk_idx, key_idx):
        scores = jnp.einsum("bihgd,bjhd->bhgij", q_blk.astype(jnp.float32), k_blk.astype(jnp.float32)) * scale
        q_pos = blk_idx * BLOCK + jnp.arange(BLOCK)
        k_pos = key_idx * BLOCK + jnp.arange(BLOCK)
        return jnp.where(q_pos[:, None] >= k_pos[None, :], scores, NEG_BIG)

    def forward_block(inputs):
        q_blk, blk_idx = inputs

        def loop_body(key_idx, carry):
            m_run, l_run, acc_run = carry
            k_blk = lax.dynamic_index_in_dim(k_blocks, key_idx, 1, keepdims=False)
            v_blk = lax.dynamic_index_in_dim(v_blocks, key_idx, 1, keepdims=False)
            scores = block_scores(q_blk, k_blk, blk_idx, key_idx)
            m_new = jnp.maximum(m_run, scores.max(axis=-1))
            rescale = jnp.exp(m_run - m_new)
            weights = jnp.exp(scores - m_new[..., None])
            l_new = l_run * rescale + weights.sum(axis=-1)
            w_half = weights.astype(jnp.bfloat16).astype(jnp.float32)
            acc_new = acc_run * rescale[..., None] + jnp.einsum("bhgij,bjhd->bhgid", w_half, v_blk.astype(jnp.float32))
            return m_new, l_new, acc_new

        init_carry = (jnp.full(stat_shape, NEG_BIG, jnp.float32), jnp.zeros(stat_shape, jnp.float32), jnp.zeros(stat_shape + (HEAD_DIM,), jnp.float32))
        m_fin, l_fin, acc_fin = lax.fori_loop(0, blk_idx + 1, loop_body, init_carry)
        out_blk = jnp.transpose((acc_fin / l_fin[..., None]).astype(jnp.bfloat16), (0, 3, 1, 2, 4))
        return out_blk, m_fin + jnp.log(l_fin)

    out_lead, lse_lead = lax.map(forward_block, (q_lead, blk_ids))

    def backward_block(carry, inputs):
        dk_acc, dv_acc = carry
        q_blk, do_blk, out_blk, lse_blk, blk_idx = inputs
        q_f = q_blk.astype(jnp.float32)
        do_f = do_blk.astype(jnp.float32)
        delta_row = jnp.einsum("bihgd,bihgd->bhgi", do_f, out_blk.astype(jnp.float32))

        def loop_body(key_idx, inner):
            dq_run, dk_run, dv_run = inner
            k_blk = lax.dynamic_index_in_dim(k_blocks, key_idx, 1, keepdims=False)
            v_blk = lax.dynamic_index_in_dim(v_blocks, key_idx, 1, keepdims=False)
            scores = block_scores(q_blk, k_blk, blk_idx, key_idx)
            weights = jnp.exp(scores - lse_blk[..., None])
            w_half = weights.astype(jnp.bfloat16).astype(jnp.float32)
            dp_blk = jnp.einsum("bihgd,bjhd->bhgij", do_f, v_blk.astype(jnp.float32))
            ds_half = (weights * (dp_blk - delta_row[..., None])).astype(jnp.bfloat16).astype(jnp.float32)
            dq_run = dq_run + jnp.einsum("bhgij,bjhd->bihgd", ds_half, k_blk.astype(jnp.float32))
            dk_old = lax.dynamic_index_in_dim(dk_run, key_idx, 1, keepdims=False)
            dv_old = lax.dynamic_index_in_dim(dv_run, key_idx, 1, keepdims=False)
            dk_new = dk_old + jnp.einsum("bhgij,bihgd->bjhd", ds_half, q_f)
            dv_new = dv_old + jnp.einsum("bhgij,bihgd->bjhd", w_half, do_f)
            dk_run = lax.dynamic_update_index_in_dim(dk_run, dk_new, key_idx, 1)
            dv_run = lax.dynamic_update_index_in_dim(dv_run, dv_new, key_idx, 1)
            return dq_run, dk_run, dv_run

        dq_blk, dk_acc, dv_acc = lax.fori_loop(0, blk_idx + 1, loop_body, (jnp.zeros(q_f.shape, jnp.float32), dk_acc, dv_acc))
        return (dk_acc, dv_acc), dq_blk

    acc_zero = jnp.zeros((BATCH, n_blocks, BLOCK, n_kv, HEAD_DIM), jnp.float32)
    grads, dq_lead = lax.scan(backward_block, (acc_zero, acc_zero), (q_lead, do_lead, out_lead, lse_lead, blk_ids))
    attn_out = jnp.moveaxis(out_lead, 0, 1).reshape(BATCH, SEQ, HQ, HEAD_DIM)
    grad_q = (jnp.moveaxis(dq_lead, 0, 1) * scale).astype(jnp.bfloat16).reshape(BATCH, SEQ, HQ, HEAD_DIM)
    grad_k = (grads[0] * scale).astype(jnp.bfloat16).reshape(BATCH, SEQ, n_kv, HEAD_DIM)
    grad_v = grads[1].astype(jnp.bfloat16).reshape(BATCH, SEQ, n_kv, HEAD_DIM)
    return attn_out, grad_q, grad_k, grad_v
```

```python
import functools
import math

import jax
import jax.numpy as jnp
from jax import lax
from jax.experimental import pallas as pl
from jax.experimental.pallas import tpu as pltpu
from jax.sharding import PartitionSpec as P

MESH = pl.DeviceIdType.MESH
NEG_BIG = -1e30
NT = (((1,), (1,)), ((), ()))
F32 = jnp.float32
BF16 = jnp.bfloat16


def dot(a, b):
    return jnp.dot(a, b, preferred_element_type=F32)


def dot_nt(a, b):
    return lax.dot_general(a, b, NT, preferred_element_type=F32)


def kernel(n_chip, n_grp, scale, q_ref, do_ref, k_ref, v_ref, o_ref, dq_ref, dkv_ref,
           q_in, do_in, kv, kt, vt, acc, part, o_st, dq_st, fin, s_buf, o_acc, dq_acc,
           send, recv, self_sem):
    n_dev = 2 * n_chip
    me = lax.axis_index("ctx")
    chip, core = me // 2, me % 2
    mate = 2 * chip + 1 - core
    c_len = kv.shape[2]
    rows = q_in.shape[1]
    half = rows // n_grp
    scale2 = scale * math.log2(math.e)

    barrier = pltpu.get_barrier_semaphore()

    def greet(s, _):
        pl.semaphore_signal(barrier, inc=1, device_id={"ctx": lax.rem(me + s, n_dev)}, device_id_type=MESH)
        return 0

    lax.fori_loop(1, n_dev, greet, 0)
    pl.semaphore_wait(barrier, n_dev - 1)

    def far_chip(n, sign):
        step = (2 * lax.rem(n, 2) - 1) * ((n + 1) // 2)
        return lax.rem(chip + sign * step + n_chip, n_chip)

    def remote(src, dst, kind, s_idx, r_idx, dev):
        return pltpu.make_async_remote_copy(src_ref=src, dst_ref=dst, send_sem=send.at[kind, s_idx], recv_sem=recv.at[kind, r_idx],
                                            device_id={"ctx": dev}, device_id_type=MESH)

    def q_copy(c, h):
        return remote(q_ref.at[c, h], q_in.at[me], 0, 2 * c + h, me, 2 * c + h)

    def do_copy(c, h):
        return remote(do_ref.at[c, h], do_in.at[me], 1, 2 * c + h, me, 2 * c + h)

    def kv_copy(c, h):
        return remote((k_ref, v_ref)[h].at[c], kv.at[h, me], 2, 2 * c + h, me, 2 * c + h)

    def fw_copy(i):
        return remote(kv.at[core, i], kv.at[core, i], 3, i, i, mate)

    def o_copy(i):
        return remote(o_st.at[i], o_ref.at[chip, core], 4, i, me, i)

    def dq_copy(i):
        return remote(dq_st.at[i], dq_ref.at[chip, core], 5, i, me, i)

    def fin_copy(i):
        return remote(fin.at[i], dkv_ref.at[core, chip], 6, i, me, i)

    part_copy = remote(acc.at[1 - core], part, 7, 0, 0, mate)

    def landed(dst, kind, i):
        return remote(dst, dst, kind, i, i, mate)

    def own(h):
        return (pltpu.make_async_copy(q_ref.at[chip, h], q_in.at[me], self_sem.at[0]),
                pltpu.make_async_copy(do_ref.at[chip, h], do_in.at[me], self_sem.at[1]),
                pltpu.make_async_copy((k_ref, v_ref)[h].at[chip], kv.at[h, me], self_sem.at[2]))

    for h in range(2):
        @pl.when(core == h)
        def _():
            kv_copy(chip, 1 - h).start()
            for cp in own(h):
                cp.start()

    def send_kv(n, _):
        c = far_chip(n, 1)
        for h in range(2):
            kv_copy(c, h).start()
        return 0

    lax.fori_loop(1, n_chip, send_kv, 0)

    for h in range(2):
        @pl.when(core == h)
        def _():
            q_copy(chip, 1 - h).start()
            do_copy(chip, 1 - h).start()

    def send_q(n, _):
        c = far_chip(n, 1)
        for h in range(2):
            q_copy(c, h).start()
            do_copy(c, h).start()
        return 0

    lax.fori_loop(1, n_chip, send_q, 0)

    acc[...] = jnp.zeros(acc.shape, F32)

    for h in range(2):
        @pl.when(core == h)
        def _():
            for cp in own(h):
                cp.wait()

    def source(n):
        return 2 * far_chip(n // 2, -1) + lax.rem(n, 2)

    def hand_over(n, _):
        i = source(n)

        @pl.when(i != me)
        def _():
            landed(kv.at[core, i], 2, i).wait_recv()

        fw_copy(i).start()
        return 0

    lax.fori_loop(0, n_dev, hand_over, 0)

    def turn(i, _):
        landed(kv.at[1 - core, i], 3, i).wait_recv()
        kt[i] = kv[0, i].astype(F32).T.astype(BF16)
        vt[i] = kv[1, i].astype(F32).T.astype(BF16)
        return 0

    lax.fori_loop(0, n_dev, turn, 0)

    def tile(n, _):
        i = source(n)

        @pl.when(i != me)
        def _():
            landed(q_in.at[i], 0, i).wait_recv()
            landed(do_in.at[i], 1, i).wait_recv()

        key_pos = lax.broadcasted_iota(jnp.int32, (c_len, rows), 0)
        q_pos = lax.broadcasted_iota(jnp.int32, (c_len, rows), 1) // n_grp + core * half
        x = jnp.where(key_pos <= q_pos, dot_nt(kv[0, i], q_in[i]) * scale2, NEG_BIG)
        s_buf[i] = x
        m = jnp.max(x, axis=0, keepdims=True)
        p = jnp.exp2(x - m)
        l = jnp.sum(p, axis=0, keepdims=True)
        o_acc[...] = dot(vt[i], p.astype(BF16))

        def forward(j, carry):
            m, l = carry
            x = dot_nt(kv[0, j], q_in[i]) * scale2
            s_buf[j] = x
            m_new = jnp.maximum(m, jnp.max(x, axis=0, keepdims=True))
            a = jnp.exp2(m - m_new)
            p = jnp.exp2(x - m_new)
            l = l * a + jnp.sum(p, axis=0, keepdims=True)
            o_acc[...] = o_acc[...] * a + dot(vt[j], p.astype(BF16))
            return m_new, l

        m, l = lax.fori_loop(0, i, forward, (m, l))
        o_half = (o_acc[...] * (1.0 / l)).astype(BF16)
        o_full = o_half.astype(F32)
        o_st[i] = o_full.T.astype(BF16)
        lse = m + jnp.log2(l)
        delta = jnp.sum(do_in[i].astype(F32).T * o_full, axis=0, keepdims=True)
        dq_acc[...] = jnp.zeros(dq_acc.shape, F32)

        @pl.when(i != me)
        def _():
            o_copy(i).start()

        def backward(j, _):
            p = jnp.exp2(s_buf[j] - lse)
            dp = dot_nt(kv[1, j], do_in[i])
            ds = (p * (dp - delta)).astype(BF16)
            acc[1, j] += dot(p.astype(BF16), do_in[i])
            acc[0, j] += dot(ds, q_in[i])
            dq_acc[...] += dot(kt[j], ds)
            return 0

        lax.fori_loop(0, i + 1, backward, 0)
        dq_st[i] = (dq_acc[...] * scale).T.astype(BF16)

        @pl.when(i != me)
        def _():
            dq_copy(i).start()

        return 0

    lax.fori_loop(0, n_dev, tile, 0)

    own_o = pltpu.make_async_copy(o_st.at[me], o_ref.at[chip, core], self_sem.at[3])
    own_dq = pltpu.make_async_copy(dq_st.at[me], dq_ref.at[chip, core], self_sem.at[4])
    own_fin = pltpu.make_async_copy(fin.at[me], dkv_ref.at[core, chip], self_sem.at[5])
    own_o.start()
    own_dq.start()

    part_copy.start()
    part_copy.wait()
    factor = jnp.where(core == 0, scale, 1.0).astype(F32)

    def finish(n, _):
        i = source(n)
        fin[i] = ((acc[core, i] + part[i]) * factor).astype(BF16)

        @pl.when(i != me)
        def _():
            fin_copy(i).start()

        return 0

    lax.fori_loop(0, n_dev, finish, 0)
    own_fin.start()

    def drain_in(i, _):
        fw_copy(i).wait_send()

        @pl.when(i != me)
        def _():
            c, h = i // 2, lax.rem(i, 2)
            landed(q_in.at[i], 0, i).wait_send()
            landed(do_in.at[i], 1, i).wait_send()
            landed(kv.at[0, i], 2, i).wait_send()
            o_copy(i).wait_send()
            dq_copy(i).wait_send()
            fin_copy(i).wait_send()
            landed(o_ref.at[c, h], 4, i).wait_recv()
            landed(dq_ref.at[c, h], 5, i).wait_recv()
            landed(dkv_ref.at[h, c], 6, i).wait_recv()

        return 0

    lax.fori_loop(0, n_dev, drain_in, 0)
    own_o.wait()
    own_dq.wait()
    own_fin.wait()


def solution(mesh):
    part_spec = P("dp", "ctx")
    n_ctx = mesh.shape["ctx"]
    n_chip = n_ctx // 2

    def local_step(queries, keys, values, grad_out):
        n_batch, c_len, n_q, d_head = queries.shape
        assert keys.shape[2] == 1 and n_batch == n_chip
        rows = c_len * n_q // 2
        q_shape = (n_batch, 2, rows, d_head)
        kv_shape = (n_batch, c_len, d_head)
        hbm = pl.BlockSpec(memory_space=pl.ANY)
        vmem = pltpu.VMEM
        out, grad_q, grad_kv = pl.pallas_call(
            functools.partial(kernel, n_chip, n_q, d_head ** -0.5),
            out_shape=(jax.ShapeDtypeStruct(q_shape, BF16), jax.ShapeDtypeStruct(q_shape, BF16), jax.ShapeDtypeStruct((2,) + kv_shape, BF16)),
            in_specs=[hbm] * 4,
            out_specs=(hbm,) * 3,
            scratch_shapes=[
                vmem((n_ctx, rows, d_head), BF16),
                vmem((n_ctx, rows, d_head), BF16),
                vmem((2, n_ctx, c_len, d_head), BF16),
                vmem((n_ctx, d_head, c_len), BF16),
                vmem((n_ctx, d_head, c_len), BF16),
                vmem((2, n_ctx, c_len, d_head), F32),
                vmem((n_ctx, c_len, d_head), F32),
                vmem((n_ctx, rows, d_head), BF16),
                vmem((n_ctx, rows, d_head), BF16),
                vmem((n_ctx, c_len, d_head), BF16),
                vmem((n_ctx, c_len, rows), F32),
                vmem((d_head, rows), F32),
                vmem((d_head, rows), F32),
                pltpu.SemaphoreType.DMA((8, n_ctx)),
                pltpu.SemaphoreType.DMA((8, n_ctx)),
                pltpu.SemaphoreType.DMA((6,)),
            ],
            compiler_params=pltpu.CompilerParams(collective_id=0, has_side_effects=True, vmem_limit_bytes=60 * 2 ** 20),
        )(queries.reshape(q_shape), grad_out.reshape(q_shape), keys.reshape(kv_shape), values.reshape(kv_shape))
        return (out.reshape(queries.shape), grad_q.reshape(queries.shape), grad_kv[0].reshape(keys.shape), grad_kv[1].reshape(values.shape))

    return jax.shard_map(local_step, mesh=mesh, in_specs=(part_spec,) * 4, out_specs=(part_spec,) * 4, check_vma=False)
```

```python
import functools
import math

import jax
import jax.numpy as jnp
from jax import lax
from jax.experimental import pallas as pl
from jax.experimental.pallas import tpu as pltpu
from jax.sharding import PartitionSpec as P

MESH = pl.DeviceIdType.MESH
NEG_BIG = -1e30
NT = (((1,), (1,)), ((), ()))
F32 = jnp.float32
BF16 = jnp.bfloat16
Q, DO, KV, RELAY, SHARE, O, DQ, FIN, PART, N_KIND = range(10)


def dot(a, b):
    return jnp.dot(a, b, preferred_element_type=F32)


def dot_nt(a, b):
    return lax.dot_general(a, b, NT, preferred_element_type=F32)


def kernel(n_chip, n_grp, scale, q_ref, do_ref, k_ref, v_ref, o_ref, dq_ref, dk_ref, dv_ref,
           q_in, do_in, kv, kt, vt, acc, part, cross, o_st, dq_st, fin, s_buf, o_acc, dq_acc,
           send, recv, self_sem):
    n_dev = 2 * n_chip
    n_far = n_chip // 2
    me = lax.axis_index("ctx")
    chip, core = me // 2, me % 2
    mate = 2 * chip + 1 - core
    d_head = q_in.shape[-1]
    cols, keys = q_in.shape[1] * q_in.shape[2], kv.shape[3] * kv.shape[4]
    scale2 = scale * math.log2(math.e)

    barrier = pltpu.get_barrier_semaphore()

    def greet(s, _):
        pl.semaphore_signal(barrier, inc=1, device_id={"ctx": lax.rem(me + s, n_dev)}, device_id_type=MESH)
        return 0

    lax.fori_loop(1, n_dev, greet, 0)
    pl.semaphore_wait(barrier, n_dev - 1)

    def wrap(c):
        return lax.rem(c + 2 * n_chip, n_chip)

    def sign(r):
        return 1 - 2 * r

    def seq(r, c):
        return wrap(c - r)

    def remote(src, dst, kind, s_idx, r_idx, dev):
        return pltpu.make_async_remote_copy(src_ref=src, dst_ref=dst, send_sem=send.at[kind, s_idx], recv_sem=recv.at[kind, r_idx],
                                            device_id={"ctx": dev}, device_id_type=MESH)

    def landed(dst, kind, i):
        return remote(dst, dst, kind, i, i, mate)

    def out_q(r, d, h, src, dst, kind):
        c = wrap(chip + sign(r) * d)
        slot = n_far * r + d
        return remote(src.at[seq(r, c), h], dst.at[slot, core], kind, 2 * slot + h, 2 * slot + core, 2 * c + h)

    def out_kv(r, d, h):
        c = wrap(chip + sign(r) * d)
        slot = n_far * r + d
        return remote((k_ref, v_ref)[h].at[seq(r, c)], kv.at[r, h, chip, core], KV, 2 * slot + h, 2 * slot + core, 2 * c + h)

    def relay(r, d, g):
        z = wrap(chip - sign(r) * d)
        t = 2 * (n_far * r + d) + g
        return remote(kv.at[r, core, z, g], kv.at[1 - r, core, z, g], RELAY, t, t, 2 * wrap(chip + sign(r)) + core)

    def share(r, z):
        return remote(kv.at[r, core, z], kv.at[r, core, z], SHARE, n_chip * r + z, n_chip * r + z, mate)

    def back(r, d, g, src, dst, kind):
        z = wrap(chip - sign(r) * d)
        slot = n_far * r + d
        return remote(src.at[slot, g], dst, kind, 2 * slot + g, 2 * slot + core, 2 * z + g)

    def part_copy(r):
        return remote(acc.at[r, 1 - core], part.at[r], PART, r, r, mate)

    def cross_copy(r, d):
        z = wrap(chip + sign(r) * (d + 1))
        i = 2 + n_far * r + d
        return remote(acc.at[r, core, z], cross.at[1 - r, d], PART, i, i, 2 * wrap(chip + sign(r)) + core)

    def own(r, h):
        slot = n_far * r
        b = seq(r, chip)
        return (pltpu.make_async_copy((k_ref, v_ref)[h].at[b], kv.at[r, h, chip, h], self_sem.at[KV, r]),
                pltpu.make_async_copy(q_ref.at[b, h], q_in.at[slot, h], self_sem.at[Q, r]),
                pltpu.make_async_copy(do_ref.at[b, h], do_in.at[slot, h], self_sem.at[DO, r]))

    def send_rows(d):
        for r in range(2):
            for h in range(2):
                out_q(r, d, h, q_ref, q_in, Q).start()
                out_q(r, d, h, do_ref, do_in, DO).start()

    for h in range(2):
        @pl.when(core == h)
        def _():
            for r in range(2):
                out_kv(r, 0, 1 - h).start()
                for cp in own(r, h):
                    cp.start()

    def send_kv(d, _):
        for r in range(2):
            for h in range(2):
                out_kv(r, d, h).start()
        return 0

    lax.fori_loop(1, n_far, send_kv, 0)

    for h in range(2):
        @pl.when(core == h)
        def _():
            for r in range(2):
                out_q(r, 0, 1 - h, q_ref, q_in, Q).start()
                out_q(r, 0, 1 - h, do_ref, do_in, DO).start()
            for r in range(2):
                for cp in own(r, h):
                    cp.wait()

    def pass_on(d, _):
        for r in range(2):
            for g in range(2):
                @pl.when(jnp.logical_or(d > 0, core != g))
                def _():
                    landed(kv.at[r, core, wrap(chip - sign(r) * d), g], KV, 2 * (n_far * r + d) + g).wait_recv()

                relay(r, d, g).start()
            share(r, wrap(chip - sign(r) * d)).start()
        return 0

    lax.fori_loop(0, n_far, pass_on, 0)

    def send_far(d, _):
        send_rows(d)
        return 0

    lax.fori_loop(1, n_far, send_far, 0)

    acc[...] = jnp.zeros(acc.shape, F32)

    def take(d, _):
        for r in range(2):
            z = wrap(chip + sign(r) * (d + 1))
            for g in range(2):
                landed(kv.at[r, core, z, g], RELAY, 2 * (n_far * (1 - r) + d) + g).wait_recv()
            share(r, z).start()
        return 0

    lax.fori_loop(0, n_far, take, 0)

    def turn(z, _):
        for r in range(2):
            landed(kv.at[r, 1 - core, z], SHARE, n_chip * r + z).wait_recv()
            kt[r, z] = kv[r, 0, z].reshape(keys, d_head).astype(F32).T.astype(BF16)
            vt[r, z] = kv[r, 1, z].reshape(keys, d_head).astype(F32).T.astype(BF16)
        return 0

    lax.fori_loop(0, n_chip, turn, 0)

    def add_part(r):
        part_copy(r).wait_recv()

        def add(z, _):
            acc[r, core, z] += part[r, z]
            return 0

        lax.fori_loop(0, n_chip, add, 0)

        def go(d, _):
            cross_copy(r, d).start()
            return 0

        lax.fori_loop(0, n_far, go, 0)

    def tile(n, _):
        r, d = lax.rem(n, 2), n // 2
        z = wrap(chip - sign(r) * d)
        slot = n_far * r + d

        @pl.when(n == 2 * n_far - 1)
        def _():
            part_copy(0).start()

        for g in range(2):
            @pl.when(jnp.logical_or(d > 0, core != g))
            def _():
                landed(q_in.at[slot, g], Q, 2 * slot + g).wait_recv()
                landed(do_in.at[slot, g], DO, 2 * slot + g).wait_recv()

        def q_rows():
            return q_in[slot].reshape(cols, d_head)

        def do_rows():
            return do_in[slot].reshape(cols, d_head)

        def block(kind, j):
            return kv[r, kind, j].reshape(keys, d_head)

        col = lax.broadcasted_iota(jnp.int32, (1, cols), 1)
        q_pos = col // (cols // 2) * (keys // 2) + core * (keys // 4) + lax.rem(col, cols // 2) // n_grp
        key_pos = lax.broadcasted_iota(jnp.int32, (keys, cols), 0)
        x = jnp.where(key_pos <= q_pos, dot_nt(block(0, z), q_rows()) * scale2, NEG_BIG)
        s_buf[z] = x
        m = jnp.max(x, axis=0, keepdims=True)
        p = jnp.exp2(x - m)
        l = jnp.sum(p, axis=0, keepdims=True)
        o_acc[...] = dot(vt[r, z], p.astype(BF16))

        def forward(j, carry):
            m, l = carry
            x = dot_nt(block(0, j), q_rows()) * scale2
            s_buf[j] = x
            m_new = jnp.maximum(m, jnp.max(x, axis=0, keepdims=True))
            a = jnp.exp2(m - m_new)
            p = jnp.exp2(x - m_new)
            l = l * a + jnp.sum(p, axis=0, keepdims=True)
            o_acc[...] = o_acc[...] * a + dot(vt[r, j], p.astype(BF16))
            return m_new, l

        m, l = lax.fori_loop(0, z, forward, (m, l))
        o_full = (o_acc[...] * (1.0 / l)).astype(BF16).astype(F32)
        o_st[slot] = o_full.T.astype(BF16).reshape(o_st.shape[1:])
        lse = m + jnp.log2(l)
        delta = jnp.sum(do_rows().astype(F32).T * o_full, axis=0, keepdims=True)
        dq_acc[...] = jnp.zeros(dq_acc.shape, F32)

        for g in range(2):
            @pl.when(jnp.logical_or(d > 0, core != g))
            def _():
                back(r, d, g, o_st, o_ref.at[seq(r, chip), core], O).start()

        def backward(j, _):
            p = jnp.exp2(s_buf[j] - lse)
            dp = dot_nt(block(1, j), do_rows())
            ds = (p * (dp - delta)).astype(BF16)
            acc[r, 1, j] += dot(p.astype(BF16), do_rows())
            acc[r, 0, j] += dot(ds, q_rows())
            dq_acc[...] += dot(kt[r, j], ds)
            return 0

        lax.fori_loop(0, z + 1, backward, 0)
        dq_st[slot] = (dq_acc[...] * scale).T.astype(BF16).reshape(dq_st.shape[1:])

        for g in range(2):
            @pl.when(jnp.logical_or(d > 0, core != g))
            def _():
                back(r, d, g, dq_st, dq_ref.at[seq(r, chip), core], DQ).start()

        return 0

    lax.fori_loop(0, 2 * n_far, tile, 0)
    part_copy(1).start()

    def own_out(r, h):
        slot, b = n_far * r, seq(r, chip)
        return (pltpu.make_async_copy(o_st.at[slot, h], o_ref.at[b, h], self_sem.at[O, r]),
                pltpu.make_async_copy(dq_st.at[slot, h], dq_ref.at[b, h], self_sem.at[DQ, r]),
                pltpu.make_async_copy(fin.at[slot, h], (dk_ref, dv_ref)[h].at[b], self_sem.at[FIN, r]))

    for h in range(2):
        @pl.when(core == h)
        def _():
            for r in range(2):
                own_out(r, h)[0].start()
                own_out(r, h)[1].start()

    add_part(0)
    add_part(1)

    factor = jnp.where(core == 0, scale, 1.0).astype(F32)

    for r in (1, 0):
        def finish(d, _):
            slot = n_far * r + d
            landed(cross.at[r, d], PART, 2 + n_far * (1 - r) + d).wait_recv()
            total = acc[r, core, wrap(chip - sign(r) * d)] + cross[r, d]
            fin[slot] = (total * factor).astype(BF16).reshape(fin.shape[1:])
            for h in range(2):
                for g in range(2):
                    @pl.when(jnp.logical_and(core == h, jnp.logical_or(d > 0, h != g)))
                    def _():
                        back(r, d, g, fin, (dk_ref, dv_ref)[h].at[seq(r, chip)], FIN).start()

            return 0

        lax.fori_loop(0, n_far, finish, 0)

    for h in range(2):
        @pl.when(core == h)
        def _():
            for r in range(2):
                own_out(r, h)[2].start()

    def drain(d, _):
        for r in range(2):
            slot = n_far * r + d
            c = wrap(chip + sign(r) * d)
            cross_copy(r, d).wait_send()
            share(r, d).wait_send()
            share(r, d + n_far).wait_send()
            for h in range(2):
                t = 2 * slot + h
                relay(r, d, h).wait_send()

                @pl.when(jnp.logical_or(d > 0, core != h))
                def _():
                    landed(q_in.at[slot, h], Q, t).wait_send()
                    landed(do_in.at[slot, h], DO, t).wait_send()
                    landed(kv.at[r, 0, d, h], KV, t).wait_send()
                    landed(o_st.at[slot, h], O, t).wait_send()
                    landed(dq_st.at[slot, h], DQ, t).wait_send()
                    landed(fin.at[slot, h], FIN, t).wait_send()
                    landed(o_ref.at[seq(r, c), h], O, t).wait_recv()
                    landed(dq_ref.at[seq(r, c), h], DQ, t).wait_recv()
                    landed((dk_ref, dv_ref)[h].at[seq(r, c)], FIN, t).wait_recv()

        return 0

    lax.fori_loop(0, n_far, drain, 0)
    for r in range(2):
        part_copy(r).wait_send()
    for h in range(2):
        @pl.when(core == h)
        def _():
            for r in range(2):
                for cp in own_out(r, h):
                    cp.wait()


def solution(mesh):
    part_spec = P("dp", "ctx")
    n_ctx = mesh.shape["ctx"]
    n_chip = n_ctx // 2
    n_far = n_chip // 2

    def local_step(queries, keys, values, grad_out):
        n_batch, c_len, n_q, d_head = queries.shape
        assert keys.shape[2] == 1 and n_batch == n_chip
        rows = c_len * n_q // 2
        q_shape = (n_batch, 2, rows, d_head)
        kv_shape = (n_batch, c_len, d_head)
        hbm = pl.BlockSpec(memory_space=pl.ANY)
        vmem = pltpu.VMEM
        tiles = vmem((2 * n_far, 2, rows, d_head), BF16)
        out, grad_q, grad_k, grad_v = pl.pallas_call(
            functools.partial(kernel, n_chip, n_q, d_head ** -0.5),
            out_shape=tuple(jax.ShapeDtypeStruct(s, BF16) for s in (q_shape, q_shape, kv_shape, kv_shape)),
            in_specs=[hbm] * 4,
            out_specs=(hbm,) * 4,
            scratch_shapes=[
                tiles,
                tiles,
                vmem((2, 2, n_chip, 2, c_len, d_head), BF16),
                vmem((2, n_chip, d_head, 2 * c_len), BF16),
                vmem((2, n_chip, d_head, 2 * c_len), BF16),
                vmem((2, 2, n_chip, 2 * c_len, d_head), F32),
                vmem((2, n_chip, 2 * c_len, d_head), F32),
                vmem((2, n_far, 2 * c_len, d_head), F32),
                tiles,
                tiles,
                vmem((2 * n_far, 2, c_len, d_head), BF16),
                vmem((n_chip, 2 * c_len, 2 * rows), F32),
                vmem((d_head, 2 * rows), F32),
                vmem((d_head, 2 * rows), F32),
                pltpu.SemaphoreType.DMA((N_KIND, n_ctx)),
                pltpu.SemaphoreType.DMA((N_KIND, n_ctx)),
                pltpu.SemaphoreType.DMA((N_KIND, 2)),
            ],
            compiler_params=pltpu.CompilerParams(collective_id=0, has_side_effects=True, vmem_limit_bytes=62 * 2 ** 20),
        )(queries.reshape(q_shape), grad_out.reshape(q_shape), keys.reshape(kv_shape), values.reshape(kv_shape))
        return (out.reshape(queries.shape), grad_q.reshape(queries.shape), grad_k.reshape(keys.shape), grad_v.reshape(values.shape))

    return jax.shard_map(local_step, mesh=mesh, in_specs=(part_spec,) * 4, out_specs=(part_spec,) * 4, check_vma=False)
```

```python
import functools
import math

import jax
import jax.numpy as jnp
from jax import lax
from jax.experimental import pallas as pl
from jax.experimental.pallas import tpu as pltpu
from jax.sharding import PartitionSpec as P

MESH = pl.DeviceIdType.MESH
NEG_BIG = -1e30
NT = (((1,), (1,)), ((), ()))
F32 = jnp.float32
BF16 = jnp.bfloat16
Q, DO, KV, RELAY, SHARE, O, DQ, FIN, PART, N_KIND = range(10)


def dot(a, b):
    return jnp.dot(a, b, preferred_element_type=F32)


def dot_nt(a, b):
    return lax.dot_general(a, b, NT, preferred_element_type=F32)


def kernel(n_chip, n_grp, scale, q_ref, do_ref, k_ref, v_ref, o_ref, dq_ref, dk_ref, dv_ref,
           q_in, do_in, kv, kt, vt, acc, part, cross, o_st, dq_st, fin, s_buf, o_acc, dq_acc,
           send, recv, self_sem):
    n_far = n_chip // 2
    me = lax.axis_index("ctx")
    chip, core = me // 2, me % 2
    mate = 2 * chip + 1 - core
    d_head = q_in.shape[-1]
    cols, keys = q_in.shape[1] * q_in.shape[2], kv.shape[3] * kv.shape[4]
    scale2 = scale * math.log2(math.e)

    barrier = pltpu.get_barrier_semaphore()

    def wrap(c):
        return lax.rem(c + 2 * n_chip, n_chip)

    pl.semaphore_signal(barrier, inc=1, device_id={"ctx": mate}, device_id_type=MESH)

    def greet(d, _):
        for c in (wrap(chip + d), wrap(chip - d)):
            for h in range(2):
                pl.semaphore_signal(barrier, inc=1, device_id={"ctx": 2 * c + h}, device_id_type=MESH)
        return 0

    lax.fori_loop(1, n_far, greet, 0)
    pl.semaphore_wait(barrier, 4 * n_far - 3)

    def sign(r):
        return 1 - 2 * r

    def seq(r, c):
        return wrap(c - r)

    def last(r, c):
        if r == 0:
            return jnp.where(c >= n_far - 1, c, n_chip - 1)
        return jnp.where(c <= n_chip - n_far, c + n_far - 1, n_chip - 1)

    def reads(r, c, z):
        return z <= last(r, c)

    def remote(src, dst, kind, s_idx, r_idx, dev):
        return pltpu.make_async_remote_copy(src_ref=src, dst_ref=dst, send_sem=send.at[kind, s_idx], recv_sem=recv.at[kind, r_idx],
                                            device_id={"ctx": dev}, device_id_type=MESH)

    def landed(dst, kind, i):
        return remote(dst, dst, kind, i, i, mate)

    def out_q(r, d, h, src, dst, kind):
        c = wrap(chip + sign(r) * d)
        slot = n_far * r + d
        return remote(src.at[seq(r, c), h], dst.at[slot, core], kind, 2 * slot + h, 2 * slot + core, 2 * c + h)

    def out_kv(r, d, h):
        c = wrap(chip + sign(r) * d)
        slot = n_far * r + d
        return remote((k_ref, v_ref)[h].at[seq(r, c)], kv.at[r, h, chip, core], KV, 2 * slot + h, 2 * slot + core, 2 * c + h)

    def relay(r, d, g):
        z = wrap(chip - sign(r) * d)
        t = 2 * (n_far * r + d) + g
        return remote(kv.at[r, core, z, g], kv.at[1 - r, core, z, g], RELAY, t, t, 2 * wrap(chip + sign(r)) + core)

    def relayed(r, d):
        return reads(1 - r, wrap(chip + sign(r)), wrap(chip - sign(r) * d))

    def share(r, z):
        return remote(kv.at[r, core, z], kv.at[r, core, z], SHARE, n_chip * r + z, n_chip * r + z, mate)

    def back(r, d, g, src, dst, kind):
        z = wrap(chip - sign(r) * d)
        slot = n_far * r + d
        return remote(src.at[slot, g], dst, kind, 2 * slot + g, 2 * slot + core, 2 * z + g)

    def part_copy(r):
        return remote(acc.at[r, 1 - core], part.at[r], PART, r, r, mate)

    def cross_copy(r, d):
        z = wrap(chip + sign(r) * (d + 1))
        i = 2 + n_far * r + d
        return remote(acc.at[r, core, z], cross.at[1 - r, d], PART, i, i, 2 * wrap(chip + sign(r)) + core)

    def own(r, h):
        slot = n_far * r
        b = seq(r, chip)
        return (pltpu.make_async_copy((k_ref, v_ref)[h].at[b], kv.at[r, h, chip, h], self_sem.at[KV, r]),
                pltpu.make_async_copy(q_ref.at[b, h], q_in.at[slot, h], self_sem.at[Q, r]),
                pltpu.make_async_copy(do_ref.at[b, h], do_in.at[slot, h], self_sem.at[DO, r]))

    def send_rows(d):
        for r in range(2):
            for h in range(2):
                out_q(r, d, h, q_ref, q_in, Q).start()
                out_q(r, d, h, do_ref, do_in, DO).start()

    for h in range(2):
        @pl.when(core == h)
        def _():
            for r in range(2):
                out_kv(r, 0, 1 - h).start()
                for cp in own(r, h):
                    cp.start()

    def send_kv(n, _):
        d = n_far - n
        for r in range(2):
            for h in range(2):
                out_kv(r, d, h).start()
        return 0

    lax.fori_loop(1, n_far, send_kv, 0)

    for h in range(2):
        @pl.when(core == h)
        def _():
            for r in range(2):
                out_q(r, 0, 1 - h, q_ref, q_in, Q).start()
                out_q(r, 0, 1 - h, do_ref, do_in, DO).start()
            for r in range(2):
                for cp in own(r, h):
                    cp.wait()

    def pass_on(d, _):
        for r in range(2):
            for g in range(2):
                @pl.when(jnp.logical_or(d > 0, core != g))
                def _():
                    landed(kv.at[r, core, wrap(chip - sign(r) * d), g], KV, 2 * (n_far * r + d) + g).wait_recv()

                @pl.when(relayed(r, d))
                def _():
                    relay(r, d, g).start()
            share(r, wrap(chip - sign(r) * d)).start()
        return 0

    lax.fori_loop(0, n_far, pass_on, 0)

    def send_far(d, _):
        send_rows(d)
        return 0

    lax.fori_loop(1, n_far, send_far, 0)

    acc[...] = jnp.zeros(acc.shape, F32)

    def take(d, _):
        for r in range(2):
            z = wrap(chip + sign(r) * (d + 1))

            @pl.when(reads(r, chip, z))
            def _():
                for g in range(2):
                    landed(kv.at[r, core, z, g], RELAY, 2 * (n_far * (1 - r) + d) + g).wait_recv()
                share(r, z).start()

        return 0

    lax.fori_loop(0, n_far, take, 0)

    def turn(z, _):
        for r in range(2):
            @pl.when(reads(r, chip, z))
            def _():
                landed(kv.at[r, 1 - core, z], SHARE, n_chip * r + z).wait_recv()
                kt[r, z] = kv[r, 0, z].reshape(keys, d_head).astype(F32).T.astype(BF16)
                vt[r, z] = kv[r, 1, z].reshape(keys, d_head).astype(F32).T.astype(BF16)

        return 0

    lax.fori_loop(0, n_chip, turn, 0)

    def add_part(r):
        part_copy(r).wait_recv()

        def add(z, _):
            acc[r, core, z] += part[r, z]
            return 0

        lax.fori_loop(0, n_chip, add, 0)

        def go(n, _):
            d = n_far - 1 - n

            @pl.when(reads(r, chip, wrap(chip + sign(r) * (d + 1))))
            def _():
                cross_copy(r, d).start()

            return 0

        lax.fori_loop(0, n_far, go, 0)

    def tile(n, _):
        r, d = lax.rem(n, 2), n // 2
        z = wrap(chip - sign(r) * d)
        slot = n_far * r + d

        @pl.when(n == 2 * n_far - 1)
        def _():
            part_copy(0).start()

        for g in range(2):
            @pl.when(jnp.logical_or(d > 0, core != g))
            def _():
                landed(q_in.at[slot, g], Q, 2 * slot + g).wait_recv()
                landed(do_in.at[slot, g], DO, 2 * slot + g).wait_recv()

        def q_rows():
            return q_in[slot].reshape(cols, d_head)

        def do_rows():
            return do_in[slot].reshape(cols, d_head)

        def block(kind, j):
            return kv[r, kind, j].reshape(keys, d_head)

        col = lax.broadcasted_iota(jnp.int32, (1, cols), 1)
        q_pos = col // (cols // 2) * (keys // 2) + core * (keys // 4) + lax.rem(col, cols // 2) // n_grp
        key_pos = lax.broadcasted_iota(jnp.int32, (keys, cols), 0)
        x = jnp.where(key_pos <= q_pos, dot_nt(block(0, z), q_rows()) * scale2, NEG_BIG)
        s_buf[z] = x
        m = jnp.max(x, axis=0, keepdims=True)
        p = jnp.exp2(x - m)
        l = jnp.sum(p, axis=0, keepdims=True)
        o_acc[...] = dot(vt[r, z], p.astype(BF16))

        def forward(j, carry):
            m, l = carry
            x = dot_nt(block(0, j), q_rows()) * scale2
            s_buf[j] = x
            m_new = jnp.maximum(m, jnp.max(x, axis=0, keepdims=True))
            a = jnp.exp2(m - m_new)
            p = jnp.exp2(x - m_new)
            l = l * a + jnp.sum(p, axis=0, keepdims=True)
            o_acc[...] = o_acc[...] * a + dot(vt[r, j], p.astype(BF16))
            return m_new, l

        m, l = lax.fori_loop(0, z, forward, (m, l))
        o_full = (o_acc[...] * (1.0 / l)).astype(BF16).astype(F32)
        o_st[slot] = o_full.T.astype(BF16).reshape(o_st.shape[1:])
        lse = m + jnp.log2(l)
        delta = jnp.sum(do_rows().astype(F32).T * o_full, axis=0, keepdims=True)
        dq_acc[...] = jnp.zeros(dq_acc.shape, F32)

        for g in range(2):
            @pl.when(jnp.logical_or(d > 0, core != g))
            def _():
                back(r, d, g, o_st, o_ref.at[seq(r, chip), core], O).start()

        def backward(j, _):
            p = jnp.exp2(s_buf[j] - lse)
            dp = dot_nt(block(1, j), do_rows())
            ds = (p * (dp - delta)).astype(BF16)
            acc[r, 1, j] += dot(p.astype(BF16), do_rows())
            acc[r, 0, j] += dot(ds, q_rows())
            dq_acc[...] += dot(kt[r, j], ds)
            return 0

        lax.fori_loop(0, z + 1, backward, 0)
        dq_st[slot] = (dq_acc[...] * scale).T.astype(BF16).reshape(dq_st.shape[1:])

        for g in range(2):
            @pl.when(jnp.logical_or(d > 0, core != g))
            def _():
                back(r, d, g, dq_st, dq_ref.at[seq(r, chip), core], DQ).start()

        return 0

    lax.fori_loop(0, 2 * n_far, tile, 0)
    part_copy(1).start()

    def own_out(r, h):
        slot, b = n_far * r, seq(r, chip)
        return (pltpu.make_async_copy(o_st.at[slot, h], o_ref.at[b, h], self_sem.at[O, r]),
                pltpu.make_async_copy(dq_st.at[slot, h], dq_ref.at[b, h], self_sem.at[DQ, r]),
                pltpu.make_async_copy(fin.at[slot, h], (dk_ref, dv_ref)[h].at[b], self_sem.at[FIN, r]))

    for h in range(2):
        @pl.when(core == h)
        def _():
            for r in range(2):
                own_out(r, h)[0].start()
                own_out(r, h)[1].start()

    add_part(0)
    add_part(1)

    factor = jnp.where(core == 0, scale, 1.0).astype(F32)

    def finish(n, _):
        d = n_far - 1 - n
        for r in range(2):
            slot = n_far * r + d
            z = wrap(chip - sign(r) * d)

            @pl.when(relayed(r, d))
            def _():
                landed(cross.at[r, d], PART, 2 + n_far * (1 - r) + d).wait_recv()
                acc[r, core, z] += cross[r, d]

            fin[slot] = (acc[r, core, z] * factor).astype(BF16).reshape(fin.shape[1:])
            for h in range(2):
                for g in range(2):
                    @pl.when(jnp.logical_and(core == h, jnp.logical_or(d > 0, h != g)))
                    def _():
                        back(r, d, g, fin, (dk_ref, dv_ref)[h].at[seq(r, chip)], FIN).start()
        return 0

    lax.fori_loop(0, n_far, finish, 0)

    for h in range(2):
        @pl.when(core == h)
        def _():
            for r in range(2):
                own_out(r, h)[2].start()

    def drain(d, _):
        for r in range(2):
            slot = n_far * r + d
            c = wrap(chip + sign(r) * d)
            for z in (d, d + n_far):
                @pl.when(reads(r, chip, z))
                def _():
                    share(r, z).wait_send()

            @pl.when(reads(r, chip, wrap(chip + sign(r) * (d + 1))))
            def _():
                cross_copy(r, d).wait_send()

            for h in range(2):
                t = 2 * slot + h

                @pl.when(relayed(r, d))
                def _():
                    relay(r, d, h).wait_send()

                @pl.when(jnp.logical_or(d > 0, core != h))
                def _():
                    landed(q_in.at[slot, h], Q, t).wait_send()
                    landed(do_in.at[slot, h], DO, t).wait_send()
                    landed(kv.at[r, 0, d, h], KV, t).wait_send()
                    landed(o_st.at[slot, h], O, t).wait_send()
                    landed(dq_st.at[slot, h], DQ, t).wait_send()
                    landed(fin.at[slot, h], FIN, t).wait_send()
                    landed(o_ref.at[seq(r, c), h], O, t).wait_recv()
                    landed(dq_ref.at[seq(r, c), h], DQ, t).wait_recv()
                    landed((dk_ref, dv_ref)[h].at[seq(r, c)], FIN, t).wait_recv()

        return 0

    lax.fori_loop(0, n_far, drain, 0)
    for r in range(2):
        part_copy(r).wait_send()
    for h in range(2):
        @pl.when(core == h)
        def _():
            for r in range(2):
                for cp in own_out(r, h):
                    cp.wait()


def copy_kernel(*refs):
    n = (len(refs) - 2) // 3
    src, dst, buf, sem_in, sem_out = refs[:n], refs[n:2 * n], refs[2 * n:3 * n], refs[-2], refs[-1]
    pieces = [(a, b) for a in range(n) for b in range(src[a].shape[0])]
    ins = [pltpu.make_async_copy(src[a].at[b], buf[a].at[b], sem_in.at[a, b]) for a, b in pieces]
    outs = [pltpu.make_async_copy(buf[a].at[b], dst[a].at[b], sem_out.at[a, b]) for a, b in pieces]
    for cp in ins:
        cp.start()
    for cp_in, cp_out in zip(ins, outs):
        cp_in.wait()
        cp_out.start()
    for cp in outs:
        cp.wait()


def settle(*arrays):
    hbm = pl.BlockSpec(memory_space=pl.ANY)
    n = len(arrays)
    sems = pltpu.SemaphoreType.DMA((n, arrays[0].shape[0]))
    return pl.pallas_call(
        copy_kernel,
        out_shape=tuple(jax.ShapeDtypeStruct(a.shape, a.dtype) for a in arrays),
        in_specs=[hbm] * n,
        out_specs=(hbm,) * n,
        scratch_shapes=[pltpu.VMEM(a.shape, a.dtype) for a in arrays] + [sems, sems],
    )(*arrays)


def solution(mesh):
    part_spec = P("dp", "ctx")
    n_ctx = mesh.shape["ctx"]
    n_chip = n_ctx // 2
    n_far = n_chip // 2

    def local_step(queries, keys, values, grad_out):
        n_batch, c_len, n_q, d_head = queries.shape
        assert keys.shape[2] == 1 and n_batch == n_chip
        rows = c_len * n_q // 2
        q_shape = (n_batch, 2, rows, d_head)
        kv_shape = (n_batch, c_len, d_head)
        hbm = pl.BlockSpec(memory_space=pl.ANY)
        vmem = pltpu.VMEM
        tiles = vmem((2 * n_far, 2, rows, d_head), BF16)
        out, grad_q, grad_k, grad_v = pl.pallas_call(
            functools.partial(kernel, n_chip, n_q, d_head ** -0.5),
            out_shape=tuple(jax.ShapeDtypeStruct(s, BF16) for s in (q_shape, q_shape, kv_shape, kv_shape)),
            in_specs=[hbm] * 4,
            out_specs=(hbm,) * 4,
            scratch_shapes=[
                tiles,
                tiles,
                vmem((2, 2, n_chip, 2, c_len, d_head), BF16),
                vmem((2, n_chip, d_head, 2 * c_len), BF16),
                vmem((2, n_chip, d_head, 2 * c_len), BF16),
                vmem((2, 2, n_chip, 2 * c_len, d_head), F32),
                vmem((2, n_chip, 2 * c_len, d_head), F32),
                vmem((2, n_far, 2 * c_len, d_head), F32),
                tiles,
                tiles,
                vmem((2 * n_far, 2, c_len, d_head), BF16),
                vmem((n_chip, 2 * c_len, 2 * rows), F32),
                vmem((d_head, 2 * rows), F32),
                vmem((d_head, 2 * rows), F32),
                pltpu.SemaphoreType.DMA((N_KIND, n_ctx)),
                pltpu.SemaphoreType.DMA((N_KIND, n_ctx)),
                pltpu.SemaphoreType.DMA((N_KIND, 2)),
            ],
            compiler_params=pltpu.CompilerParams(collective_id=0, has_side_effects=True, vmem_limit_bytes=62 * 2 ** 20),
        )(queries.reshape(q_shape), grad_out.reshape(q_shape), keys.reshape(kv_shape), values.reshape(kv_shape))
        out, grad_q, grad_k, grad_v = settle(out, grad_q, grad_k, grad_v)
        return (out.reshape(queries.shape), grad_q.reshape(queries.shape), grad_k.reshape(keys.shape), grad_v.reshape(values.shape))

    return jax.shard_map(local_step, mesh=mesh, in_specs=(part_spec,) * 4, out_specs=(part_spec,) * 4, check_vma=False)
```

```python
import functools
import math

import jax
import jax.numpy as jnp
from jax import lax
from jax.experimental import pallas as pl
from jax.experimental.pallas import tpu as pltpu
from jax.sharding import PartitionSpec as P

MESH = pl.DeviceIdType.MESH
NEG_BIG = -1e30
NT = (((1,), (1,)), ((), ()))
F32 = jnp.float32
BF16 = jnp.bfloat16
Q, DO, KV, RELAY, SHARE, O, DQ, FIN, PART, HOME, N_KIND = range(11)
H_Q, H_DO, H_K, H_V, H_O, H_DQ, H_FIN, H_PART = range(0, 16, 2)


def dot(a, b):
    return jnp.dot(a, b, preferred_element_type=F32)


def dot_nt(a, b):
    return lax.dot_general(a, b, NT, preferred_element_type=F32)


def kernel(n_chip, n_grp, scale, q_ref, do_ref, k_ref, v_ref, o_ref, dq_ref, dk_ref, dv_ref,
           q_in, do_in, kv, kt, vt, acc, part, cross, o_st, dq_st, fin, s_buf, o_acc, dq_acc,
           h_q, h_do, h_kv, h_o, h_dq, h_acc, h_part, h_cross, h_fin,
           send, recv, self_sem, home_sem):
    n_far = n_chip // 2
    me = lax.axis_index("ctx")
    chip, core = me // 2, me % 2
    mate = 2 * chip + 1 - core
    d_head = q_in.shape[-1]
    cols, keys = q_in.shape[1] * q_in.shape[2], kv.shape[3] * kv.shape[4]
    scale2 = scale * math.log2(math.e)

    barrier = pltpu.get_barrier_semaphore()

    def wrap(c):
        return lax.rem(c + 2 * n_chip, n_chip)

    pl.semaphore_signal(barrier, inc=1, device_id={"ctx": mate}, device_id_type=MESH)

    def greet(d, _):
        for c in (wrap(chip + d), wrap(chip - d)):
            for h in range(2):
                pl.semaphore_signal(barrier, inc=1, device_id={"ctx": 2 * c + h}, device_id_type=MESH)
        return 0

    lax.fori_loop(1, n_far, greet, 0)
    pl.semaphore_wait(barrier, 4 * n_far - 3)

    def sign(r):
        return 1 - 2 * r

    def seq(r, c):
        return wrap(c - r)

    def last(r, c):
        if r == 0:
            return jnp.where(c >= n_far - 1, c, n_chip - 1)
        return jnp.where(c <= n_chip - n_far, c + n_far - 1, n_chip - 1)

    def reads(r, c, z):
        return z <= last(r, c)

    def remote(src, dst, kind, s_idx, r_idx, dev):
        return pltpu.make_async_remote_copy(src_ref=src, dst_ref=dst, send_sem=send.at[kind, s_idx], recv_sem=recv.at[kind, r_idx],
                                            device_id={"ctx": dev}, device_id_type=MESH)

    def landed(dst, kind, i):
        return remote(dst, dst, kind, i, i, mate)

    def out_q(r, d, h, src, dst, kind):
        c = wrap(chip + sign(r) * d)
        slot = n_far * r + d
        return remote(src.at[seq(r, c), h], dst.at[slot, core], kind, 2 * slot + h, 2 * slot + core, 2 * c + h)

    def out_kv(r, d, h):
        c = wrap(chip + sign(r) * d)
        slot = n_far * r + d
        return remote((k_ref, v_ref)[h].at[seq(r, c)], kv.at[r, h, chip, core], KV, 2 * slot + h, 2 * slot + core, 2 * c + h)

    def relay(r, d, g):
        z = wrap(chip - sign(r) * d)
        t = 2 * (n_far * r + d) + g
        return remote(kv.at[r, core, z, g], kv.at[1 - r, core, z, g], RELAY, t, t, 2 * wrap(chip + sign(r)) + core)

    def stays(d, z):
        return jnp.logical_and(d == n_far - 1, z == 0)

    def leaves(d, z):
        return jnp.logical_or(d < n_far - 1, z > 0)

    def relayed(r, d):
        return reads(1 - r, wrap(chip + sign(r)), wrap(chip - sign(r) * d))

    def share(r, z):
        return remote(kv.at[r, core, z], kv.at[r, core, z], SHARE, n_chip * r + z, n_chip * r + z, mate)

    def back(r, d, g, src, dst, kind):
        z = wrap(chip - sign(r) * d)
        slot = n_far * r + d
        return remote(src.at[slot, g], dst, kind, 2 * slot + g, 2 * slot + core, 2 * z + g)

    def part_copy(r):
        return remote(acc.at[r, 1 - core], part.at[r], PART, r, r, mate)

    def cross_copy(r, d):
        z = wrap(chip + sign(r) * (d + 1))
        i = 2 + n_far * r + d
        return remote(acc.at[r, core, z], cross.at[1 - r, d], PART, i, i, 2 * wrap(chip + sign(r)) + core)

    def own(r, h):
        slot = n_far * r
        b = seq(r, chip)
        return (pltpu.make_async_copy((k_ref, v_ref)[h].at[b], kv.at[r, h, chip, h], self_sem.at[KV, r]),
                pltpu.make_async_copy(q_ref.at[b, h], q_in.at[slot, h], self_sem.at[Q, r]),
                pltpu.make_async_copy(do_ref.at[b, h], do_in.at[slot, h], self_sem.at[DO, r]))

    def send_rows(d):
        for r in range(2):
            for h in range(2):
                out_q(r, d, h, q_ref, q_in, Q).start()
                out_q(r, d, h, do_ref, do_in, DO).start()

    for h in range(2):
        @pl.when(core == h)
        def _():
            for r in range(2):
                out_kv(r, 0, 1 - h).start()
                for cp in own(r, h):
                    cp.start()

    def send_kv(n, _):
        d = n_far - n
        for r in range(2):
            for h in range(2):
                out_kv(r, d, h).start()
        return 0

    lax.fori_loop(1, n_far, send_kv, 0)

    for h in range(2):
        @pl.when(core == h)
        def _():
            for r in range(2):
                out_q(r, 0, 1 - h, q_ref, q_in, Q).start()
                out_q(r, 0, 1 - h, do_ref, do_in, DO).start()
            for r in range(2):
                for cp in own(r, h):
                    cp.wait()

    def pass_on(d, _):
        for r in range(2):
            for g in range(2):
                @pl.when(jnp.logical_or(d > 0, core != g))
                def _():
                    landed(kv.at[r, core, wrap(chip - sign(r) * d), g], KV, 2 * (n_far * r + d) + g).wait_recv()

                @pl.when(relayed(r, d))
                def _():
                    relay(r, d, g).start()
            share(r, wrap(chip - sign(r) * d)).start()
        return 0

    lax.fori_loop(0, n_far, pass_on, 0)

    def send_far(d, _):
        @pl.when(leaves(d, chip))
        def _():
            send_rows(d)

        return 0

    lax.fori_loop(1, n_far, send_far, 0)

    def diagonal(k_rows, q_rows):
        col = lax.broadcasted_iota(jnp.int32, (1, cols), 1)
        q_pos = col // (cols // 2) * (keys // 2) + core * (keys // 4) + lax.rem(col, cols // 2) // n_grp
        key_pos = lax.broadcasted_iota(jnp.int32, (keys, cols), 0)
        return jnp.where(key_pos <= q_pos, dot_nt(k_rows, q_rows) * scale2, NEG_BIG)

    def to_mate(src, dst, i):
        return remote(src, dst, HOME, i, i, mate)

    def stay(src, dst, i):
        return pltpu.make_async_copy(src, dst, home_sem.at[i])

    def home_in(t, move, half):
        b = n_far - 1 + t
        return (move(q_ref.at[b, half], h_q.at[t, core], H_Q + t), move(do_ref.at[b, half], h_do.at[t, core], H_DO + t),
                move(k_ref.at[b], h_kv.at[t, 0, core], H_K + t), move(v_ref.at[b], h_kv.at[t, 1, core], H_V + t))

    def home_out(t, move, half):
        b = n_far - 1 + t
        return (move(h_o.at[t, half], o_ref.at[b, core], H_O + t), move(h_dq.at[t, half], dq_ref.at[b, core], H_DQ + t))

    def home_part(t):
        return to_mate(h_acc.at[t, 1 - core], h_part.at[t], H_PART + t)

    def home_fin(t, h):
        out = (dk_ref, dv_ref)[h].at[n_far - 1 + t]
        return stay(h_fin.at[t, h], out, H_FIN + t), to_mate(h_fin.at[t, 1 - h], out, H_FIN + t)

    @pl.when(chip == 0)
    def _():
        for t in range(2):
            for cp in home_in(t, to_mate, 1 - core) + home_in(t, stay, core):
                cp.start()
        for t in range(2):
            for cp in home_in(t, stay, core):
                cp.wait()
            for cp in home_in(t, to_mate, 1 - core):
                cp.wait()

        def home_tile(t, _):
            q_rows, do_rows = h_q[t].reshape(cols, d_head), h_do[t].reshape(cols, d_head)
            k_rows, v_rows = h_kv[t, 0].reshape(keys, d_head), h_kv[t, 1].reshape(keys, d_head)
            x = diagonal(k_rows, q_rows)
            s_buf[0] = x
            m = jnp.max(x, axis=0, keepdims=True)
            p = jnp.exp2(x - m)
            l = jnp.sum(p, axis=0, keepdims=True)
            o = dot(v_rows.astype(F32).T.astype(BF16), p.astype(BF16))
            o_full = (o * (1.0 / l)).astype(BF16).astype(F32)
            h_o[t] = o_full.T.astype(BF16).reshape(h_o.shape[1:])
            delta = jnp.sum(do_rows.astype(F32).T * o_full, axis=0, keepdims=True)
            p = jnp.exp2(s_buf[0] - (m + jnp.log2(l)))
            ds = (p * (dot_nt(v_rows, do_rows) - delta)).astype(BF16)
            h_acc[t, 1] = dot(p.astype(BF16), do_rows)
            h_acc[t, 0] = dot(ds, q_rows)
            dq = dot(k_rows.astype(F32).T.astype(BF16), ds)
            h_dq[t] = (dq * scale).T.astype(BF16).reshape(h_dq.shape[1:])
            return 0

        lax.fori_loop(0, 2, home_tile, 0)
        for t in range(2):
            for cp in home_out(t, to_mate, 1 - core) + home_out(t, stay, core):
                cp.start()
            home_part(t).start()

    acc[...] = jnp.zeros(acc.shape, F32)

    def take(d, _):
        for r in range(2):
            z = wrap(chip + sign(r) * (d + 1))

            @pl.when(reads(r, chip, z))
            def _():
                for g in range(2):
                    landed(kv.at[r, core, z, g], RELAY, 2 * (n_far * (1 - r) + d) + g).wait_recv()
                share(r, z).start()

        return 0

    lax.fori_loop(0, n_far, take, 0)

    def turn(z, _):
        for r in range(2):
            @pl.when(reads(r, chip, z))
            def _():
                landed(kv.at[r, 1 - core, z], SHARE, n_chip * r + z).wait_recv()
                kt[r, z] = kv[r, 0, z].reshape(keys, d_head).astype(F32).T.astype(BF16)
                vt[r, z] = kv[r, 1, z].reshape(keys, d_head).astype(F32).T.astype(BF16)

        return 0

    lax.fori_loop(0, n_chip, turn, 0)

    def add_part(r):
        part_copy(r).wait_recv()

        def add(z, _):
            acc[r, core, z] += part[r, z]
            return 0

        lax.fori_loop(0, n_chip, add, 0)

        def go(n, _):
            d = n_far - 1 - n

            @pl.when(reads(r, chip, wrap(chip + sign(r) * (d + 1))))
            def _():
                cross_copy(r, d).start()

            return 0

        lax.fori_loop(0, n_far, go, 0)

    def tile(n, _):
        r, d = lax.rem(n, 2), n // 2
        z = wrap(chip - sign(r) * d)
        slot = n_far * r + d

        @pl.when(n == 2 * n_far - 1)
        def _():
            part_copy(0).start()

        @pl.when(leaves(d, z))
        def _():
            work(r, d, z, slot)

        return 0

    def work(r, d, z, slot):

        for g in range(2):
            @pl.when(jnp.logical_or(d > 0, core != g))
            def _():
                landed(q_in.at[slot, g], Q, 2 * slot + g).wait_recv()
                landed(do_in.at[slot, g], DO, 2 * slot + g).wait_recv()

        def q_rows():
            return q_in[slot].reshape(cols, d_head)

        def do_rows():
            return do_in[slot].reshape(cols, d_head)

        def block(kind, j):
            return kv[r, kind, j].reshape(keys, d_head)

        x = diagonal(block(0, z), q_rows())
        s_buf[z] = x
        m = jnp.max(x, axis=0, keepdims=True)
        p = jnp.exp2(x - m)
        l = jnp.sum(p, axis=0, keepdims=True)
        o_acc[...] = dot(vt[r, z], p.astype(BF16))

        def forward(j, carry):
            m, l = carry
            x = dot_nt(block(0, j), q_rows()) * scale2
            s_buf[j] = x
            m_new = jnp.maximum(m, jnp.max(x, axis=0, keepdims=True))
            a = jnp.exp2(m - m_new)
            p = jnp.exp2(x - m_new)
            l = l * a + jnp.sum(p, axis=0, keepdims=True)
            o_acc[...] = o_acc[...] * a + dot(vt[r, j], p.astype(BF16))
            return m_new, l

        m, l = lax.fori_loop(0, z, forward, (m, l))
        o_full = (o_acc[...] * (1.0 / l)).astype(BF16).astype(F32)
        o_st[slot] = o_full.T.astype(BF16).reshape(o_st.shape[1:])
        lse = m + jnp.log2(l)
        delta = jnp.sum(do_rows().astype(F32).T * o_full, axis=0, keepdims=True)
        dq_acc[...] = jnp.zeros(dq_acc.shape, F32)

        for g in range(2):
            @pl.when(jnp.logical_or(d > 0, core != g))
            def _():
                back(r, d, g, o_st, o_ref.at[seq(r, chip), core], O).start()

        def backward(j, _):
            p = jnp.exp2(s_buf[j] - lse)
            dp = dot_nt(block(1, j), do_rows())
            ds = (p * (dp - delta)).astype(BF16)
            acc[r, 1, j] += dot(p.astype(BF16), do_rows())
            acc[r, 0, j] += dot(ds, q_rows())
            dq_acc[...] += dot(kt[r, j], ds)
            return 0

        lax.fori_loop(0, z + 1, backward, 0)
        dq_st[slot] = (dq_acc[...] * scale).T.astype(BF16).reshape(dq_st.shape[1:])

        for g in range(2):
            @pl.when(jnp.logical_or(d > 0, core != g))
            def _():
                back(r, d, g, dq_st, dq_ref.at[seq(r, chip), core], DQ).start()

    lax.fori_loop(0, 2 * n_far, tile, 0)
    part_copy(1).start()

    def own_out(r, h):
        slot, b = n_far * r, seq(r, chip)
        return (pltpu.make_async_copy(o_st.at[slot, h], o_ref.at[b, h], self_sem.at[O, r]),
                pltpu.make_async_copy(dq_st.at[slot, h], dq_ref.at[b, h], self_sem.at[DQ, r]),
                pltpu.make_async_copy(fin.at[slot, h], (dk_ref, dv_ref)[h].at[b], self_sem.at[FIN, r]))

    for h in range(2):
        @pl.when(core == h)
        def _():
            for r in range(2):
                own_out(r, h)[0].start()
                own_out(r, h)[1].start()

    add_part(0)
    add_part(1)

    factor = jnp.where(core == 0, scale, 1.0).astype(F32)

    def home_cross(r):
        return remote(acc.at[r, core, 0], h_cross.at[r], PART, 2 + 2 * n_far + r, 2 + 2 * n_far + r, core)

    def finish(n, _):
        d = n_far - 1 - n
        for r in range(2):
            slot = n_far * r + d
            z = wrap(chip - sign(r) * d)

            @pl.when(relayed(r, d))
            def _():
                landed(cross.at[r, d], PART, 2 + n_far * (1 - r) + d).wait_recv()
                acc[r, core, z] += cross[r, d]

            fin[slot] = (acc[r, core, z] * factor).astype(BF16).reshape(fin.shape[1:])
            for h in range(2):
                for g in range(2):
                    @pl.when(jnp.logical_and(leaves(d, z), jnp.logical_and(core == h, jnp.logical_or(d > 0, h != g))))
                    def _():
                        back(r, d, g, fin, (dk_ref, dv_ref)[h].at[seq(r, chip)], FIN).start()

            @pl.when(stays(d, z))
            def _():
                home_cross(r).start()

        return 0

    lax.fori_loop(0, n_far, finish, 0)

    for h in range(2):
        @pl.when(core == h)
        def _():
            for r in range(2):
                own_out(r, h)[2].start()

    @pl.when(chip == 0)
    def _():
        for t in range(2):
            home_part(t).wait()
            landed(h_cross.at[t], PART, 2 + 2 * n_far + t).wait_recv()
            total = h_acc[t, core] + h_part[t] + h_cross[t]
            h_fin[t] = (total * factor).astype(BF16).reshape(h_fin.shape[1:])
        for h in range(2):
            @pl.when(core == h)
            def _():
                for t in range(2):
                    for cp in home_fin(t, h):
                        cp.start()
                for t in range(2):
                    kept, sent = home_fin(t, h)
                    kept.wait()
                    sent.wait_send()
                    landed((dk_ref, dv_ref)[1 - h].at[n_far - 1 + t], HOME, H_FIN + t).wait_recv()
        for t in range(2):
            for cp in home_out(t, to_mate, 1 - core) + home_out(t, stay, core):
                cp.wait()

    def drain(d, _):
        for r in range(2):
            slot = n_far * r + d
            c = wrap(chip + sign(r) * d)
            for z in (d, d + n_far):
                @pl.when(reads(r, chip, z))
                def _():
                    share(r, z).wait_send()

            @pl.when(reads(r, chip, wrap(chip + sign(r) * (d + 1))))
            def _():
                cross_copy(r, d).wait_send()

            for h in range(2):
                t = 2 * slot + h

                @pl.when(relayed(r, d))
                def _():
                    relay(r, d, h).wait_send()

                away = jnp.logical_or(d > 0, core != h)

                @pl.when(away)
                def _():
                    landed(kv.at[r, 0, d, h], KV, t).wait_send()

                @pl.when(jnp.logical_and(away, leaves(d, chip)))
                def _():
                    landed(q_in.at[slot, h], Q, t).wait_send()
                    landed(do_in.at[slot, h], DO, t).wait_send()
                    landed(o_ref.at[seq(r, c), h], O, t).wait_recv()
                    landed(dq_ref.at[seq(r, c), h], DQ, t).wait_recv()
                    landed((dk_ref, dv_ref)[h].at[seq(r, c)], FIN, t).wait_recv()

                @pl.when(jnp.logical_and(away, leaves(d, wrap(chip - sign(r) * d))))
                def _():
                    landed(o_st.at[slot, h], O, t).wait_send()
                    landed(dq_st.at[slot, h], DQ, t).wait_send()
                    landed(fin.at[slot, h], FIN, t).wait_send()

            @pl.when(stays(d, wrap(chip - sign(r) * d)))
            def _():
                home_cross(r).wait_send()

        return 0

    lax.fori_loop(0, n_far, drain, 0)
    for r in range(2):
        part_copy(r).wait_send()
    for h in range(2):
        @pl.when(core == h)
        def _():
            for r in range(2):
                for cp in own_out(r, h):
                    cp.wait()


def copy_kernel(*refs):
    n = (len(refs) - 2) // 3
    src, dst, buf, sem_in, sem_out = refs[:n], refs[n:2 * n], refs[2 * n:3 * n], refs[-2], refs[-1]
    pieces = [(a, b) for a in range(n) for b in range(src[a].shape[0])]
    ins = [pltpu.make_async_copy(src[a].at[b], buf[a].at[b], sem_in.at[a, b]) for a, b in pieces]
    outs = [pltpu.make_async_copy(buf[a].at[b], dst[a].at[b], sem_out.at[a, b]) for a, b in pieces]
    for cp in ins:
        cp.start()
    for cp_in, cp_out in zip(ins, outs):
        cp_in.wait()
        cp_out.start()
    for cp in outs:
        cp.wait()


def settle(*arrays):
    hbm = pl.BlockSpec(memory_space=pl.ANY)
    n = len(arrays)
    sems = pltpu.SemaphoreType.DMA((n, arrays[0].shape[0]))
    return pl.pallas_call(
        copy_kernel,
        out_shape=tuple(jax.ShapeDtypeStruct(a.shape, a.dtype) for a in arrays),
        in_specs=[hbm] * n,
        out_specs=(hbm,) * n,
        scratch_shapes=[pltpu.VMEM(a.shape, a.dtype) for a in arrays] + [sems, sems],
    )(*arrays)


def solution(mesh):
    part_spec = P("dp", "ctx")
    n_ctx = mesh.shape["ctx"]
    n_chip = n_ctx // 2
    n_far = n_chip // 2

    def local_step(queries, keys, values, grad_out):
        n_batch, c_len, n_q, d_head = queries.shape
        assert keys.shape[2] == 1 and n_batch == n_chip
        rows = c_len * n_q // 2
        q_shape = (n_batch, 2, rows, d_head)
        kv_shape = (n_batch, c_len, d_head)
        hbm = pl.BlockSpec(memory_space=pl.ANY)
        vmem = pltpu.VMEM
        tiles = vmem((2 * n_far, 2, rows, d_head), BF16)
        out, grad_q, grad_k, grad_v = pl.pallas_call(
            functools.partial(kernel, n_chip, n_q, d_head ** -0.5),
            out_shape=tuple(jax.ShapeDtypeStruct(s, BF16) for s in (q_shape, q_shape, kv_shape, kv_shape)),
            in_specs=[hbm] * 4,
            out_specs=(hbm,) * 4,
            scratch_shapes=[
                tiles,
                tiles,
                vmem((2, 2, n_chip, 2, c_len, d_head), BF16),
                vmem((2, n_chip, d_head, 2 * c_len), BF16),
                vmem((2, n_chip, d_head, 2 * c_len), BF16),
                vmem((2, 2, n_chip, 2 * c_len, d_head), F32),
                vmem((2, n_chip, 2 * c_len, d_head), F32),
                vmem((2, n_far, 2 * c_len, d_head), F32),
                tiles,
                tiles,
                vmem((2 * n_far, 2, c_len, d_head), BF16),
                vmem((n_chip, 2 * c_len, 2 * rows), F32),
                vmem((d_head, 2 * rows), F32),
                vmem((d_head, 2 * rows), F32),
                vmem((2, 2, rows, d_head), BF16),
                vmem((2, 2, rows, d_head), BF16),
                vmem((2, 2, 2, c_len, d_head), BF16),
                vmem((2, 2, rows, d_head), BF16),
                vmem((2, 2, rows, d_head), BF16),
                vmem((2, 2, 2 * c_len, d_head), F32),
                vmem((2, 2 * c_len, d_head), F32),
                vmem((2, 2 * c_len, d_head), F32),
                vmem((2, 2, c_len, d_head), BF16),
                pltpu.SemaphoreType.DMA((N_KIND, n_ctx)),
                pltpu.SemaphoreType.DMA((N_KIND, n_ctx)),
                pltpu.SemaphoreType.DMA((N_KIND, 2)),
                pltpu.SemaphoreType.DMA((16,)),
            ],
            compiler_params=pltpu.CompilerParams(collective_id=0, has_side_effects=True, vmem_limit_bytes=62 * 2 ** 20),
        )(queries.reshape(q_shape), grad_out.reshape(q_shape), keys.reshape(kv_shape), values.reshape(kv_shape))
        out, grad_q, grad_k, grad_v = settle(out, grad_q, grad_k, grad_v)
        return (out.reshape(queries.shape), grad_q.reshape(queries.shape), grad_k.reshape(keys.shape), grad_v.reshape(values.shape))

    return jax.shard_map(local_step, mesh=mesh, in_specs=(part_spec,) * 4, out_specs=(part_spec,) * 4, check_vma=False)
```

```python
import functools
import math

import jax
import jax.numpy as jnp
from jax import lax
from jax.experimental import pallas as pl
from jax.experimental.pallas import tpu as pltpu
from jax.sharding import PartitionSpec as P

MESH = pl.DeviceIdType.MESH
NEG_BIG = -1e30
NT = (((1,), (1,)), ((), ()))
F32 = jnp.float32
BF16 = jnp.bfloat16
Q, DO, KV, RELAY, SHARE, O, DQ, FIN, PART, HOME, N_KIND = range(11)
H_Q, H_DO, H_K, H_V, H_O, H_DQ, H_FIN, H_PART = range(0, 16, 2)


def dot(a, b):
    return jnp.dot(a, b, preferred_element_type=F32)


def dot_nt(a, b):
    return lax.dot_general(a, b, NT, preferred_element_type=F32)


def kernel(n_chip, n_grp, scale, q_ref, do_ref, k_ref, v_ref, o_ref, dq_ref, dk_ref, dv_ref,
           q_in, do_in, kv, kt, vt, acc, part, cross, o_st, dq_st, fin, s_buf, o_acc, dq_acc,
           h_q, h_do, h_kv, h_o, h_dq, h_acc, h_part, h_cross, h_fin,
           send, recv, self_sem, home_sem):
    n_far = n_chip // 2
    me = lax.axis_index("ctx")
    chip, core = me // 2, me % 2
    mate = 2 * chip + 1 - core
    d_head = q_in.shape[-1]
    cols, keys = q_in.shape[1] * q_in.shape[2], kv.shape[3] * kv.shape[4]
    scale2 = scale * math.log2(math.e)

    barrier = pltpu.get_barrier_semaphore()

    def wrap(c):
        return lax.rem(c + 2 * n_chip, n_chip)

    pl.semaphore_signal(barrier, inc=1, device_id={"ctx": mate}, device_id_type=MESH)

    def greet(n, _):
        d = n_far - n
        for c in (wrap(chip + d), wrap(chip - d)):
            for h in range(2):
                pl.semaphore_signal(barrier, inc=1, device_id={"ctx": 2 * c + h}, device_id_type=MESH)
        return 0

    lax.fori_loop(1, n_far, greet, 0)
    pl.semaphore_wait(barrier, 4 * n_far - 3)

    def sign(r):
        return 1 - 2 * r

    def seq(r, c):
        return wrap(c - r)

    def last(r, c):
        if r == 0:
            return jnp.where(c >= n_far - 1, c, n_chip - 1)
        return jnp.where(c <= n_chip - n_far, c + n_far - 1, n_chip - 1)

    def reads(r, c, z):
        return z <= last(r, c)

    def remote(src, dst, kind, s_idx, r_idx, dev):
        return pltpu.make_async_remote_copy(src_ref=src, dst_ref=dst, send_sem=send.at[kind, s_idx], recv_sem=recv.at[kind, r_idx],
                                            device_id={"ctx": dev}, device_id_type=MESH)

    def landed(dst, kind, i):
        return remote(dst, dst, kind, i, i, mate)

    def out_q(r, d, h, src, dst, kind):
        c = wrap(chip + sign(r) * d)
        slot = n_far * r + d
        return remote(src.at[seq(r, c), h], dst.at[slot, core], kind, 2 * slot + h, 2 * slot + core, 2 * c + h)

    def out_kv(r, d, h):
        c = wrap(chip + sign(r) * d)
        slot = n_far * r + d
        return remote((k_ref, v_ref)[h].at[seq(r, c)], kv.at[r, h, chip, core], KV, 2 * slot + h, 2 * slot + core, 2 * c + h)

    def relay(r, d, g):
        z = wrap(chip - sign(r) * d)
        t = 2 * (n_far * r + d) + g
        return remote(kv.at[r, core, z, g], kv.at[1 - r, core, z, g], RELAY, t, t, 2 * wrap(chip + sign(r)) + core)

    def stays(d, z):
        return jnp.logical_and(d == n_far - 1, z == 0)

    def leaves(d, z):
        return jnp.logical_or(d < n_far - 1, z > 0)

    def relayed(r, d):
        return reads(1 - r, wrap(chip + sign(r)), wrap(chip - sign(r) * d))

    def share(r, z):
        return remote(kv.at[r, core, z], kv.at[r, core, z], SHARE, n_chip * r + z, n_chip * r + z, mate)

    def back(r, d, g, src, dst, kind):
        z = wrap(chip - sign(r) * d)
        slot = n_far * r + d
        return remote(src.at[slot, g], dst, kind, 2 * slot + g, 2 * slot + core, 2 * z + g)

    def part_copy(r):
        return remote(acc.at[r, 1 - core], part.at[r], PART, r, r, mate)

    def cross_copy(r, d):
        z = wrap(chip + sign(r) * (d + 1))
        i = 2 + n_far * r + d
        return remote(acc.at[r, core, z], cross.at[1 - r, d], PART, i, i, 2 * wrap(chip + sign(r)) + core)

    def own(r, h):
        slot = n_far * r
        b = seq(r, chip)
        return (pltpu.make_async_copy((k_ref, v_ref)[h].at[b], kv.at[r, h, chip, h], self_sem.at[KV, r]),
                pltpu.make_async_copy(q_ref.at[b, h], q_in.at[slot, h], self_sem.at[Q, r]),
                pltpu.make_async_copy(do_ref.at[b, h], do_in.at[slot, h], self_sem.at[DO, r]))

    def send_rows(d):
        for r in range(2):
            for h in range(2):
                out_q(r, d, h, q_ref, q_in, Q).start()
                out_q(r, d, h, do_ref, do_in, DO).start()

    for h in range(2):
        @pl.when(core == h)
        def _():
            for r in range(2):
                out_kv(r, 0, 1 - h).start()
                for cp in own(r, h):
                    cp.start()

    def send_kv(n, _):
        d = n_far - n
        for r in range(2):
            for h in range(2):
                out_kv(r, d, h).start()
        return 0

    lax.fori_loop(1, n_far, send_kv, 0)

    for h in range(2):
        @pl.when(core == h)
        def _():
            for r in range(2):
                out_q(r, 0, 1 - h, q_ref, q_in, Q).start()
                out_q(r, 0, 1 - h, do_ref, do_in, DO).start()
            for r in range(2):
                for cp in own(r, h):
                    cp.wait()

    def pass_on(d, _):
        for r in range(2):
            for g in range(2):
                @pl.when(jnp.logical_or(d > 0, core != g))
                def _():
                    landed(kv.at[r, core, wrap(chip - sign(r) * d), g], KV, 2 * (n_far * r + d) + g).wait_recv()

                @pl.when(relayed(r, d))
                def _():
                    relay(r, d, g).start()
            share(r, wrap(chip - sign(r) * d)).start()
        return 0

    lax.fori_loop(0, n_far, pass_on, 0)

    def send_far(d, _):
        @pl.when(leaves(d, chip))
        def _():
            send_rows(d)

        return 0

    lax.fori_loop(1, n_far, send_far, 0)

    def diagonal(k_rows, q_rows):
        col = lax.broadcasted_iota(jnp.int32, (1, cols), 1)
        q_pos = col // (cols // 2) * (keys // 2) + core * (keys // 4) + lax.rem(col, cols // 2) // n_grp
        key_pos = lax.broadcasted_iota(jnp.int32, (keys, cols), 0)
        return jnp.where(key_pos <= q_pos, dot_nt(k_rows, q_rows) * scale2, NEG_BIG)

    def to_mate(src, dst, i):
        return remote(src, dst, HOME, i, i, mate)

    def stay(src, dst, i):
        return pltpu.make_async_copy(src, dst, home_sem.at[i])

    def home_in(t, move, half):
        b = n_far - 1 + t
        return (move(q_ref.at[b, half], h_q.at[t, core], H_Q + t), move(do_ref.at[b, half], h_do.at[t, core], H_DO + t),
                move(k_ref.at[b], h_kv.at[t, 0, core], H_K + t), move(v_ref.at[b], h_kv.at[t, 1, core], H_V + t))

    def home_out(t, move, half):
        b = n_far - 1 + t
        return (move(h_o.at[t, half], o_ref.at[b, core], H_O + t), move(h_dq.at[t, half], dq_ref.at[b, core], H_DQ + t))

    def home_part(t):
        return to_mate(h_acc.at[t, 1 - core], h_part.at[t], H_PART + t)

    def home_fin(t, h):
        out = (dk_ref, dv_ref)[h].at[n_far - 1 + t]
        return stay(h_fin.at[t, h], out, H_FIN + t), to_mate(h_fin.at[t, 1 - h], out, H_FIN + t)

    @pl.when(chip == 0)
    def _():
        for t in range(2):
            for cp in home_in(t, to_mate, 1 - core) + home_in(t, stay, core):
                cp.start()
        for t in range(2):
            for cp in home_in(t, stay, core):
                cp.wait()
            for cp in home_in(t, to_mate, 1 - core):
                cp.wait()

        def home_tile(t, _):
            q_rows, do_rows = h_q[t].reshape(cols, d_head), h_do[t].reshape(cols, d_head)
            k_rows, v_rows = h_kv[t, 0].reshape(keys, d_head), h_kv[t, 1].reshape(keys, d_head)
            x = diagonal(k_rows, q_rows)
            s_buf[0] = x
            m = jnp.max(x, axis=0, keepdims=True)
            p = jnp.exp2(x - m)
            l = jnp.sum(p, axis=0, keepdims=True)
            o = dot(v_rows.astype(F32).T.astype(BF16), p.astype(BF16))
            o_full = (o * (1.0 / l)).astype(BF16).astype(F32)
            h_o[t] = o_full.T.astype(BF16).reshape(h_o.shape[1:])
            delta = jnp.sum(do_rows.astype(F32).T * o_full, axis=0, keepdims=True)
            p = jnp.exp2(s_buf[0] - (m + jnp.log2(l)))
            ds = (p * (dot_nt(v_rows, do_rows) - delta)).astype(BF16)
            h_acc[t, 1] = dot(p.astype(BF16), do_rows)
            h_acc[t, 0] = dot(ds, q_rows)
            dq = dot(k_rows.astype(F32).T.astype(BF16), ds)
            h_dq[t] = (dq * scale).T.astype(BF16).reshape(h_dq.shape[1:])
            return 0

        lax.fori_loop(0, 2, home_tile, 0)
        for t in range(2):
            for cp in home_out(t, to_mate, 1 - core) + home_out(t, stay, core):
                cp.start()
            home_part(t).start()

    acc[...] = jnp.zeros(acc.shape, F32)

    def take(d, _):
        for r in range(2):
            z = wrap(chip + sign(r) * (d + 1))

            @pl.when(reads(r, chip, z))
            def _():
                for g in range(2):
                    landed(kv.at[r, core, z, g], RELAY, 2 * (n_far * (1 - r) + d) + g).wait_recv()
                share(r, z).start()

        return 0

    lax.fori_loop(0, n_far, take, 0)

    def turn(z, _):
        for r in range(2):
            @pl.when(reads(r, chip, z))
            def _():
                landed(kv.at[r, 1 - core, z], SHARE, n_chip * r + z).wait_recv()
                kt[r, z] = kv[r, 0, z].reshape(keys, d_head).astype(F32).T.astype(BF16)
                vt[r, z] = kv[r, 1, z].reshape(keys, d_head).astype(F32).T.astype(BF16)

        return 0

    lax.fori_loop(0, n_chip, turn, 0)

    def add_part(r):
        part_copy(r).wait_recv()

        def add(z, _):
            acc[r, core, z] += part[r, z]
            return 0

        lax.fori_loop(0, n_chip, add, 0)

        def go(n, _):
            d = n_far - 1 - n

            @pl.when(reads(r, chip, wrap(chip + sign(r) * (d + 1))))
            def _():
                cross_copy(r, d).start()

            return 0

        lax.fori_loop(0, n_far, go, 0)

    def tile(n, _):
        r, d = lax.rem(n, 2), n // 2
        z = wrap(chip - sign(r) * d)
        slot = n_far * r + d

        @pl.when(n == 2 * n_far - 1)
        def _():
            part_copy(0).start()

        @pl.when(leaves(d, z))
        def _():
            work(r, d, z, slot)

        return 0

    def work(r, d, z, slot):

        for g in range(2):
            @pl.when(jnp.logical_or(d > 0, core != g))
            def _():
                landed(q_in.at[slot, g], Q, 2 * slot + g).wait_recv()
                landed(do_in.at[slot, g], DO, 2 * slot + g).wait_recv()

        def q_rows():
            return q_in[slot].reshape(cols, d_head)

        def do_rows():
            return do_in[slot].reshape(cols, d_head)

        def block(kind, j):
            return kv[r, kind, j].reshape(keys, d_head)

        x = diagonal(block(0, z), q_rows())
        s_buf[z] = x
        m = jnp.max(x, axis=0, keepdims=True)
        p = jnp.exp2(x - m)
        l = jnp.sum(p, axis=0, keepdims=True)
        o_acc[...] = dot(vt[r, z], p.astype(BF16))

        def forward(j, carry):
            m, l = carry
            x = dot_nt(block(0, j), q_rows()) * scale2
            s_buf[j] = x
            m_new = jnp.maximum(m, jnp.max(x, axis=0, keepdims=True))
            a = jnp.exp2(m - m_new)
            p = jnp.exp2(x - m_new)
            l = l * a + jnp.sum(p, axis=0, keepdims=True)
            o_acc[...] = o_acc[...] * a + dot(vt[r, j], p.astype(BF16))
            return m_new, l

        m, l = lax.fori_loop(0, z, forward, (m, l))
        o_full = (o_acc[...] * (1.0 / l)).astype(BF16).astype(F32)
        o_st[slot] = o_full.T.astype(BF16).reshape(o_st.shape[1:])
        lse = m + jnp.log2(l)
        delta = jnp.sum(do_rows().astype(F32).T * o_full, axis=0, keepdims=True)
        dq_acc[...] = jnp.zeros(dq_acc.shape, F32)

        for g in range(2):
            @pl.when(jnp.logical_or(d > 0, core != g))
            def _():
                back(r, d, g, o_st, o_ref.at[seq(r, chip), core], O).start()

        def backward(j, _):
            p = jnp.exp2(s_buf[j] - lse)
            dp = dot_nt(block(1, j), do_rows())
            ds = (p * (dp - delta)).astype(BF16)
            acc[r, 1, j] += dot(p.astype(BF16), do_rows())
            acc[r, 0, j] += dot(ds, q_rows())
            dq_acc[...] += dot(kt[r, j], ds)
            return 0

        lax.fori_loop(0, z + 1, backward, 0)
        dq_st[slot] = (dq_acc[...] * scale).T.astype(BF16).reshape(dq_st.shape[1:])

        for g in range(2):
            @pl.when(jnp.logical_or(d > 0, core != g))
            def _():
                back(r, d, g, dq_st, dq_ref.at[seq(r, chip), core], DQ).start()

    lax.fori_loop(0, 2 * n_far, tile, 0)
    part_copy(1).start()

    def own_out(r, h):
        slot, b = n_far * r, seq(r, chip)
        return (pltpu.make_async_copy(o_st.at[slot, h], o_ref.at[b, h], self_sem.at[O, r]),
                pltpu.make_async_copy(dq_st.at[slot, h], dq_ref.at[b, h], self_sem.at[DQ, r]),
                pltpu.make_async_copy(fin.at[slot, h], (dk_ref, dv_ref)[h].at[b], self_sem.at[FIN, r]))

    for h in range(2):
        @pl.when(core == h)
        def _():
            for r in range(2):
                own_out(r, h)[0].start()
                own_out(r, h)[1].start()

    add_part(0)
    add_part(1)

    factor = jnp.where(core == 0, scale, 1.0).astype(F32)

    def home_cross(r):
        return remote(acc.at[r, core, 0], h_cross.at[r], PART, 2 + 2 * n_far + r, 2 + 2 * n_far + r, core)

    def finish(n, _):
        d = n_far - 1 - n
        for r in range(2):
            slot = n_far * r + d
            z = wrap(chip - sign(r) * d)

            @pl.when(relayed(r, d))
            def _():
                landed(cross.at[r, d], PART, 2 + n_far * (1 - r) + d).wait_recv()
                acc[r, core, z] += cross[r, d]

            fin[slot] = (acc[r, core, z] * factor).astype(BF16).reshape(fin.shape[1:])
            for h in range(2):
                for g in range(2):
                    @pl.when(jnp.logical_and(leaves(d, z), jnp.logical_and(core == h, jnp.logical_or(d > 0, h != g))))
                    def _():
                        back(r, d, g, fin, (dk_ref, dv_ref)[h].at[seq(r, chip)], FIN).start()

            @pl.when(stays(d, z))
            def _():
                home_cross(r).start()

        return 0

    lax.fori_loop(0, n_far, finish, 0)

    for h in range(2):
        @pl.when(core == h)
        def _():
            for r in range(2):
                own_out(r, h)[2].start()

    @pl.when(chip == 0)
    def _():
        for t in range(2):
            home_part(t).wait()
            landed(h_cross.at[t], PART, 2 + 2 * n_far + t).wait_recv()
            total = h_acc[t, core] + h_part[t] + h_cross[t]
            h_fin[t] = (total * factor).astype(BF16).reshape(h_fin.shape[1:])
        for h in range(2):
            @pl.when(core == h)
            def _():
                for t in range(2):
                    for cp in home_fin(t, h):
                        cp.start()
                for t in range(2):
                    kept, sent = home_fin(t, h)
                    kept.wait()
                    sent.wait_send()
                    landed((dk_ref, dv_ref)[1 - h].at[n_far - 1 + t], HOME, H_FIN + t).wait_recv()
        for t in range(2):
            for cp in home_out(t, to_mate, 1 - core) + home_out(t, stay, core):
                cp.wait()

    def drain(d, _):
        for r in range(2):
            slot = n_far * r + d
            c = wrap(chip + sign(r) * d)
            for z in (d, d + n_far):
                @pl.when(reads(r, chip, z))
                def _():
                    share(r, z).wait_send()

            @pl.when(reads(r, chip, wrap(chip + sign(r) * (d + 1))))
            def _():
                cross_copy(r, d).wait_send()

            for h in range(2):
                t = 2 * slot + h

                @pl.when(relayed(r, d))
                def _():
                    relay(r, d, h).wait_send()

                away = jnp.logical_or(d > 0, core != h)

                @pl.when(away)
                def _():
                    landed(kv.at[r, 0, d, h], KV, t).wait_send()

                @pl.when(jnp.logical_and(away, leaves(d, chip)))
                def _():
                    landed(q_in.at[slot, h], Q, t).wait_send()
                    landed(do_in.at[slot, h], DO, t).wait_send()
                    landed(o_ref.at[seq(r, c), h], O, t).wait_recv()
                    landed(dq_ref.at[seq(r, c), h], DQ, t).wait_recv()
                    landed((dk_ref, dv_ref)[h].at[seq(r, c)], FIN, t).wait_recv()

                @pl.when(jnp.logical_and(away, leaves(d, wrap(chip - sign(r) * d))))
                def _():
                    landed(o_st.at[slot, h], O, t).wait_send()
                    landed(dq_st.at[slot, h], DQ, t).wait_send()
                    landed(fin.at[slot, h], FIN, t).wait_send()

            @pl.when(stays(d, wrap(chip - sign(r) * d)))
            def _():
                home_cross(r).wait_send()

        return 0

    lax.fori_loop(0, n_far, drain, 0)
    for r in range(2):
        part_copy(r).wait_send()
    for h in range(2):
        @pl.when(core == h)
        def _():
            for r in range(2):
                for cp in own_out(r, h):
                    cp.wait()


def copy_kernel(*refs):
    n = (len(refs) - 2) // 3
    src, dst, buf, sem_in, sem_out = refs[:n], refs[n:2 * n], refs[2 * n:3 * n], refs[-2], refs[-1]
    ins = [pltpu.make_async_copy(src[a], buf[a], sem_in.at[a]) for a in range(n)]
    outs = [pltpu.make_async_copy(buf[a], dst[a], sem_out.at[a]) for a in range(n)]
    for cp in ins:
        cp.start()
    for cp_in, cp_out in zip(ins, outs):
        cp_in.wait()
        cp_out.start()
    for cp in outs:
        cp.wait()


def settle(*arrays):
    hbm = pl.BlockSpec(memory_space=pl.ANY)
    n = len(arrays)
    sems = pltpu.SemaphoreType.DMA((n,))
    return pl.pallas_call(
        copy_kernel,
        out_shape=tuple(jax.ShapeDtypeStruct(a.shape, a.dtype) for a in arrays),
        in_specs=[hbm] * n,
        out_specs=(hbm,) * n,
        scratch_shapes=[pltpu.VMEM(a.shape, a.dtype) for a in arrays] + [sems, sems],
    )(*arrays)


def solution(mesh):
    part_spec = P("dp", "ctx")
    n_ctx = mesh.shape["ctx"]
    n_chip = n_ctx // 2
    n_far = n_chip // 2

    def local_step(queries, keys, values, grad_out):
        n_batch, c_len, n_q, d_head = queries.shape
        assert keys.shape[2] == 1 and n_batch == n_chip
        rows = c_len * n_q // 2
        q_shape = (n_batch, 2, rows, d_head)
        kv_shape = (n_batch, c_len, d_head)
        hbm = pl.BlockSpec(memory_space=pl.ANY)
        vmem = pltpu.VMEM
        tiles = vmem((2 * n_far, 2, rows, d_head), BF16)
        out, grad_q, grad_k, grad_v = pl.pallas_call(
            functools.partial(kernel, n_chip, n_q, d_head ** -0.5),
            out_shape=tuple(jax.ShapeDtypeStruct(s, BF16) for s in (q_shape, q_shape, kv_shape, kv_shape)),
            in_specs=[hbm] * 4,
            out_specs=(hbm,) * 4,
            scratch_shapes=[
                tiles,
                tiles,
                vmem((2, 2, n_chip, 2, c_len, d_head), BF16),
                vmem((2, n_chip, d_head, 2 * c_len), BF16),
                vmem((2, n_chip, d_head, 2 * c_len), BF16),
                vmem((2, 2, n_chip, 2 * c_len, d_head), F32),
                vmem((2, n_chip, 2 * c_len, d_head), F32),
                vmem((2, n_far, 2 * c_len, d_head), F32),
                tiles,
                tiles,
                vmem((2 * n_far, 2, c_len, d_head), BF16),
                vmem((n_chip, 2 * c_len, 2 * rows), F32),
                vmem((d_head, 2 * rows), F32),
                vmem((d_head, 2 * rows), F32),
                vmem((2, 2, rows, d_head), BF16),
                vmem((2, 2, rows, d_head), BF16),
                vmem((2, 2, 2, c_len, d_head), BF16),
                vmem((2, 2, rows, d_head), BF16),
                vmem((2, 2, rows, d_head), BF16),
                vmem((2, 2, 2 * c_len, d_head), F32),
                vmem((2, 2 * c_len, d_head), F32),
                vmem((2, 2 * c_len, d_head), F32),
                vmem((2, 2, c_len, d_head), BF16),
                pltpu.SemaphoreType.DMA((N_KIND, n_ctx)),
                pltpu.SemaphoreType.DMA((N_KIND, n_ctx)),
                pltpu.SemaphoreType.DMA((N_KIND, 2)),
                pltpu.SemaphoreType.DMA((16,)),
            ],
            compiler_params=pltpu.CompilerParams(collective_id=0, has_side_effects=True, vmem_limit_bytes=62 * 2 ** 20),
        )(queries.reshape(q_shape), grad_out.reshape(q_shape), keys.reshape(kv_shape), values.reshape(kv_shape))
        out, grad_q, grad_k, grad_v = settle(out, grad_q, grad_k, grad_v)
        return (out.reshape(queries.shape), grad_q.reshape(queries.shape), grad_k.reshape(keys.shape), grad_v.reshape(values.shape))

    return jax.shard_map(local_step, mesh=mesh, in_specs=(part_spec,) * 4, out_specs=(part_spec,) * 4, check_vma=False)
```

```python
import functools
import math

import jax
import jax.numpy as jnp
from jax import lax
from jax.experimental import pallas as pl
from jax.experimental.pallas import tpu as pltpu
from jax.sharding import PartitionSpec as P

MESH = pl.DeviceIdType.MESH
NEG_BIG = -1e30
NT = (((1,), (1,)), ((), ()))
F32 = jnp.float32
BF16 = jnp.bfloat16
ROWS, KV, RELAY, SHARE, OUT, FIN, PART, HOME, N_KIND = range(9)
S_Q, S_DO, S_KV, S_O, S_DQ, S_FIN, N_SELF = range(7)
H_Q, H_DO, H_K, H_V, H_O, H_DQ, H_FIN, H_PART = range(0, 16, 2)


def dot(a, b):
    return jnp.dot(a, b, preferred_element_type=F32)


def dot_nt(a, b):
    return lax.dot_general(a, b, NT, preferred_element_type=F32)


def kernel(n_chip, n_grp, scale, q_ref, do_ref, k_ref, v_ref, o_ref, dq_ref, dk_ref, dv_ref,
           q_in, do_in, kv, kt, vt, acc, part, cross, o_st, dq_st, fin, s_buf, o_acc, dq_acc,
           h_q, h_do, h_kv, h_o, h_dq, h_acc, h_part, h_cross, h_fin,
           send, recv, self_sem, home_sem):
    n_far = n_chip // 2
    me = lax.axis_index("ctx")
    chip, core = me // 2, me % 2
    mate = 2 * chip + 1 - core
    d_head = q_in.shape[-1]
    cols, keys = q_in.shape[1] * q_in.shape[2], kv.shape[3] * kv.shape[4]
    scale2 = scale * math.log2(math.e)

    barrier = pltpu.get_barrier_semaphore()

    def wrap(c):
        return lax.rem(c + 2 * n_chip, n_chip)

    pl.semaphore_signal(barrier, inc=1, device_id={"ctx": mate}, device_id_type=MESH)

    def greet(n, _):
        d = n_far - n
        for c in (wrap(chip + d), wrap(chip - d)):
            for h in range(2):
                pl.semaphore_signal(barrier, inc=1, device_id={"ctx": 2 * c + h}, device_id_type=MESH)
        return 0

    lax.fori_loop(1, n_far, greet, 0)
    pl.semaphore_wait(barrier, 4 * n_far - 3)

    def sign(r):
        return 1 - 2 * r

    def seq(r, c):
        return wrap(c - r)

    def last(r, c):
        if r == 0:
            return jnp.where(c >= n_far - 1, c, n_chip - 1)
        return jnp.where(c <= n_chip - n_far, c + n_far - 1, n_chip - 1)

    def reads(r, c, z):
        return z <= last(r, c)

    def remote(src, dst, kind, s_idx, r_idx, dev):
        return pltpu.make_async_remote_copy(src_ref=src, dst_ref=dst, send_sem=send.at[kind, s_idx], recv_sem=recv.at[kind, r_idx],
                                            device_id={"ctx": dev}, device_id_type=MESH)

    def landed(dst, kind, i):
        return remote(dst, dst, kind, i, i, mate)

    def out_q(r, d, h, src, dst, kind):
        c = wrap(chip + sign(r) * d)
        slot = n_far * r + d
        return remote(src.at[seq(r, c), h], dst.at[slot, core], kind, 2 * slot + h, 2 * slot + core, 2 * c + h)

    def out_kv(r, d, h):
        c = wrap(chip + sign(r) * d)
        slot = n_far * r + d
        return remote((k_ref, v_ref)[h].at[seq(r, c)], kv.at[r, h, chip, core], KV, 2 * slot + h, 2 * slot + core, 2 * c + h)

    def relay(r, d, g):
        z = wrap(chip - sign(r) * d)
        t = 2 * (n_far * r + d) + g
        return remote(kv.at[r, core, z, g], kv.at[1 - r, core, z, g], RELAY, t, t, 2 * wrap(chip + sign(r)) + core)

    def stays(d, z):
        return jnp.logical_and(d == n_far - 1, z == 0)

    def leaves(d, z):
        return jnp.logical_or(d < n_far - 1, z > 0)

    def relayed(r, d):
        return reads(1 - r, wrap(chip + sign(r)), wrap(chip - sign(r) * d))

    def share(r, z):
        return remote(kv.at[r, core, z], kv.at[r, core, z], SHARE, n_chip * r + z, n_chip * r + z, mate)

    def back(r, d, g, src, dst, kind):
        z = wrap(chip - sign(r) * d)
        slot = n_far * r + d
        return remote(src.at[slot, g], dst, kind, 2 * slot + g, 2 * slot + core, 2 * z + g)

    def part_copy(r):
        return remote(acc.at[r, 1 - core], part.at[r], PART, r, r, mate)

    def cross_copy(r, d):
        z = wrap(chip + sign(r) * (d + 1))
        i = 2 + n_far * r + d
        return remote(acc.at[r, core, z], cross.at[1 - r, d], PART, i, i, 2 * wrap(chip + sign(r)) + core)

    def own(r, h):
        slot = n_far * r
        b = seq(r, chip)
        return (pltpu.make_async_copy((k_ref, v_ref)[h].at[b], kv.at[r, h, chip, h], self_sem.at[S_KV, r]),
                pltpu.make_async_copy(q_ref.at[b, h], q_in.at[slot, h], self_sem.at[S_Q, r]),
                pltpu.make_async_copy(do_ref.at[b, h], do_in.at[slot, h], self_sem.at[S_DO, r]))

    def send_rows(d):
        for r in range(2):
            for h in range(2):
                out_q(r, d, h, q_ref, q_in, ROWS).start()
                out_q(r, d, h, do_ref, do_in, ROWS).start()

    for h in range(2):
        @pl.when(core == h)
        def _():
            for r in range(2):
                out_kv(r, 0, 1 - h).start()
                for cp in own(r, h):
                    cp.start()

    def send_kv(n, _):
        d = n_far - n
        for r in range(2):
            for h in range(2):
                out_kv(r, d, h).start()
        return 0

    lax.fori_loop(1, n_far, send_kv, 0)

    for h in range(2):
        @pl.when(core == h)
        def _():
            for r in range(2):
                out_q(r, 0, 1 - h, q_ref, q_in, ROWS).start()
                out_q(r, 0, 1 - h, do_ref, do_in, ROWS).start()
            for r in range(2):
                for cp in own(r, h):
                    cp.wait()

    def pass_on(d, _):
        for r in range(2):
            for g in range(2):
                @pl.when(jnp.logical_or(d > 0, core != g))
                def _():
                    landed(kv.at[r, core, wrap(chip - sign(r) * d), g], KV, 2 * (n_far * r + d) + g).wait_recv()

                @pl.when(relayed(r, d))
                def _():
                    relay(r, d, g).start()
            share(r, wrap(chip - sign(r) * d)).start()
        return 0

    lax.fori_loop(0, n_far, pass_on, 0)

    def send_far(d, _):
        @pl.when(leaves(d, chip))
        def _():
            send_rows(d)

        return 0

    lax.fori_loop(1, n_far, send_far, 0)

    def diagonal(k_rows, q_rows):
        col = lax.broadcasted_iota(jnp.int32, (1, cols), 1)
        q_pos = col // (cols // 2) * (keys // 2) + core * (keys // 4) + lax.rem(col, cols // 2) // n_grp
        key_pos = lax.broadcasted_iota(jnp.int32, (keys, cols), 0)
        return jnp.where(key_pos <= q_pos, dot_nt(k_rows, q_rows) * scale2, NEG_BIG)

    def to_mate(src, dst, i):
        return remote(src, dst, HOME, i, i, mate)

    def stay(src, dst, i):
        return pltpu.make_async_copy(src, dst, home_sem.at[i])

    def home_in(t, move, half):
        b = n_far - 1 + t
        return (move(q_ref.at[b, half], h_q.at[t, core], H_Q + t), move(do_ref.at[b, half], h_do.at[t, core], H_DO + t),
                move(k_ref.at[b], h_kv.at[t, 0, core], H_K + t), move(v_ref.at[b], h_kv.at[t, 1, core], H_V + t))

    def home_out(t, move, half):
        b = n_far - 1 + t
        return (move(h_o.at[t, half], o_ref.at[b, core], H_O + t), move(h_dq.at[t, half], dq_ref.at[b, core], H_DQ + t))

    def home_part(t):
        return to_mate(h_acc.at[t, 1 - core], h_part.at[t], H_PART + t)

    def home_fin(t, h):
        out = (dk_ref, dv_ref)[h].at[n_far - 1 + t]
        return stay(h_fin.at[t, h], out, H_FIN + t), to_mate(h_fin.at[t, 1 - h], out, H_FIN + t)

    @pl.when(chip == 0)
    def _():
        for t in range(2):
            for cp in home_in(t, to_mate, 1 - core) + home_in(t, stay, core):
                cp.start()
        for t in range(2):
            for cp in home_in(t, stay, core):
                cp.wait()
            for cp in home_in(t, to_mate, 1 - core):
                cp.wait()

        def home_tile(t, _):
            q_rows, do_rows = h_q[t].reshape(cols, d_head), h_do[t].reshape(cols, d_head)
            k_rows, v_rows = h_kv[t, 0].reshape(keys, d_head), h_kv[t, 1].reshape(keys, d_head)
            x = diagonal(k_rows, q_rows)
            s_buf[0] = x
            m = jnp.max(x, axis=0, keepdims=True)
            p = jnp.exp2(x - m)
            l = jnp.sum(p, axis=0, keepdims=True)
            o = dot(v_rows.astype(F32).T.astype(BF16), p.astype(BF16))
            o_full = (o * (1.0 / l)).astype(BF16).astype(F32)
            h_o[t] = o_full.T.astype(BF16).reshape(h_o.shape[1:])
            delta = jnp.sum(do_rows.astype(F32).T * o_full, axis=0, keepdims=True)
            p = jnp.exp2(s_buf[0] - (m + jnp.log2(l)))
            ds = (p * (dot_nt(v_rows, do_rows) - delta)).astype(BF16)
            h_acc[t, 1] = dot(p.astype(BF16), do_rows)
            h_acc[t, 0] = dot(ds, q_rows)
            dq = dot(k_rows.astype(F32).T.astype(BF16), ds)
            h_dq[t] = (dq * scale).T.astype(BF16).reshape(h_dq.shape[1:])
            return 0

        lax.fori_loop(0, 2, home_tile, 0)
        for t in range(2):
            for cp in home_out(t, to_mate, 1 - core) + home_out(t, stay, core):
                cp.start()
            home_part(t).start()

    acc[...] = jnp.zeros(acc.shape, F32)

    def take(d, _):
        for r in range(2):
            z = wrap(chip + sign(r) * (d + 1))

            @pl.when(reads(r, chip, z))
            def _():
                for g in range(2):
                    landed(kv.at[r, core, z, g], RELAY, 2 * (n_far * (1 - r) + d) + g).wait_recv()
                share(r, z).start()

        return 0

    lax.fori_loop(0, n_far, take, 0)

    def turn(z, _):
        for r in range(2):
            @pl.when(reads(r, chip, z))
            def _():
                landed(kv.at[r, 1 - core, z], SHARE, n_chip * r + z).wait_recv()
                kt[r, z] = kv[r, 0, z].reshape(keys, d_head).astype(F32).T.astype(BF16)
                vt[r, z] = kv[r, 1, z].reshape(keys, d_head).astype(F32).T.astype(BF16)

        return 0

    lax.fori_loop(0, n_chip, turn, 0)

    def add_part(r):
        part_copy(r).wait_recv()

        def add(z, _):
            acc[r, core, z] += part[r, z]
            return 0

        lax.fori_loop(0, n_chip, add, 0)

        def go(n, _):
            d = n_far - 1 - n

            @pl.when(reads(r, chip, wrap(chip + sign(r) * (d + 1))))
            def _():
                cross_copy(r, d).start()

            return 0

        lax.fori_loop(0, n_far, go, 0)

    def tile(n, _):
        r, d = lax.rem(n, 2), n // 2
        z = wrap(chip - sign(r) * d)
        slot = n_far * r + d

        @pl.when(n == 2 * n_far - 1)
        def _():
            part_copy(0).start()

        @pl.when(leaves(d, z))
        def _():
            work(r, d, z, slot)

        return 0

    def work(r, d, z, slot):

        for g in range(2):
            @pl.when(jnp.logical_or(d > 0, core != g))
            def _():
                landed(q_in.at[slot], ROWS, 2 * slot + g).wait_recv()

        def q_rows():
            return q_in[slot].reshape(cols, d_head)

        def do_rows():
            return do_in[slot].reshape(cols, d_head)

        def block(kind, j):
            return kv[r, kind, j].reshape(keys, d_head)

        x = diagonal(block(0, z), q_rows())
        s_buf[z] = x
        m = jnp.max(x, axis=0, keepdims=True)
        p = jnp.exp2(x - m)
        l = jnp.sum(p, axis=0, keepdims=True)
        o_acc[...] = dot(vt[r, z], p.astype(BF16))

        def forward(j, carry):
            m, l = carry
            x = dot_nt(block(0, j), q_rows()) * scale2
            s_buf[j] = x
            m_new = jnp.maximum(m, jnp.max(x, axis=0, keepdims=True))
            a = jnp.exp2(m - m_new)
            p = jnp.exp2(x - m_new)
            l = l * a + jnp.sum(p, axis=0, keepdims=True)
            o_acc[...] = o_acc[...] * a + dot(vt[r, j], p.astype(BF16))
            return m_new, l

        m, l = lax.fori_loop(0, z, forward, (m, l))
        o_full = (o_acc[...] * (1.0 / l)).astype(BF16).astype(F32)
        o_st[slot] = o_full.T.astype(BF16).reshape(o_st.shape[1:])
        lse = m + jnp.log2(l)
        delta = jnp.sum(do_rows().astype(F32).T * o_full, axis=0, keepdims=True)
        dq_acc[...] = jnp.zeros(dq_acc.shape, F32)

        for g in range(2):
            @pl.when(jnp.logical_or(d > 0, core != g))
            def _():
                back(r, d, g, o_st, o_ref.at[seq(r, chip), core], OUT).start()

        def backward(j, _):
            p = jnp.exp2(s_buf[j] - lse)
            dp = dot_nt(block(1, j), do_rows())
            ds = (p * (dp - delta)).astype(BF16)
            acc[r, 1, j] += dot(p.astype(BF16), do_rows())
            acc[r, 0, j] += dot(ds, q_rows())
            dq_acc[...] += dot(kt[r, j], ds)
            return 0

        lax.fori_loop(0, z + 1, backward, 0)
        dq_st[slot] = (dq_acc[...] * scale).T.astype(BF16).reshape(dq_st.shape[1:])

        for g in range(2):
            @pl.when(jnp.logical_or(d > 0, core != g))
            def _():
                back(r, d, g, dq_st, dq_ref.at[seq(r, chip), core], OUT).start()

    lax.fori_loop(0, 2 * n_far, tile, 0)
    part_copy(1).start()

    def own_out(r, h):
        slot, b = n_far * r, seq(r, chip)
        return (pltpu.make_async_copy(o_st.at[slot, h], o_ref.at[b, h], self_sem.at[S_O, r]),
                pltpu.make_async_copy(dq_st.at[slot, h], dq_ref.at[b, h], self_sem.at[S_DQ, r]),
                pltpu.make_async_copy(fin.at[slot, h], (dk_ref, dv_ref)[h].at[b], self_sem.at[S_FIN, r]))

    for h in range(2):
        @pl.when(core == h)
        def _():
            for r in range(2):
                own_out(r, h)[0].start()
                own_out(r, h)[1].start()

    add_part(0)
    add_part(1)

    factor = jnp.where(core == 0, scale, 1.0).astype(F32)

    def home_cross(r):
        return remote(acc.at[r, core, 0], h_cross.at[r], PART, 2 + 2 * n_far + r, 2 + 2 * n_far + r, core)

    def finish(n, _):
        d = n_far - 1 - n
        for r in range(2):
            slot = n_far * r + d
            z = wrap(chip - sign(r) * d)

            @pl.when(relayed(r, d))
            def _():
                landed(cross.at[r, d], PART, 2 + n_far * (1 - r) + d).wait_recv()
                acc[r, core, z] += cross[r, d]

            fin[slot] = (acc[r, core, z] * factor).astype(BF16).reshape(fin.shape[1:])
            for h in range(2):
                for g in range(2):
                    @pl.when(jnp.logical_and(leaves(d, z), jnp.logical_and(core == h, jnp.logical_or(d > 0, h != g))))
                    def _():
                        back(r, d, g, fin, (dk_ref, dv_ref)[h].at[seq(r, chip)], FIN).start()

            @pl.when(stays(d, z))
            def _():
                home_cross(r).start()

        return 0

    lax.fori_loop(0, n_far, finish, 0)

    for h in range(2):
        @pl.when(core == h)
        def _():
            for r in range(2):
                own_out(r, h)[2].start()

    @pl.when(chip == 0)
    def _():
        for t in range(2):
            home_part(t).wait()
            landed(h_cross.at[t], PART, 2 + 2 * n_far + t).wait_recv()
            total = h_acc[t, core] + h_part[t] + h_cross[t]
            h_fin[t] = (total * factor).astype(BF16).reshape(h_fin.shape[1:])
        for h in range(2):
            @pl.when(core == h)
            def _():
                for t in range(2):
                    for cp in home_fin(t, h):
                        cp.start()
                for t in range(2):
                    kept, sent = home_fin(t, h)
                    kept.wait()
                    sent.wait_send()
                    landed((dk_ref, dv_ref)[1 - h].at[n_far - 1 + t], HOME, H_FIN + t).wait_recv()
        for t in range(2):
            for cp in home_out(t, to_mate, 1 - core) + home_out(t, stay, core):
                cp.wait()

    def drain(d, _):
        for r in range(2):
            slot = n_far * r + d
            c = wrap(chip + sign(r) * d)
            for z in (d, d + n_far):
                @pl.when(reads(r, chip, z))
                def _():
                    share(r, z).wait_send()

            @pl.when(reads(r, chip, wrap(chip + sign(r) * (d + 1))))
            def _():
                cross_copy(r, d).wait_send()

            for h in range(2):
                t = 2 * slot + h

                @pl.when(relayed(r, d))
                def _():
                    relay(r, d, h).wait_send()

                away = jnp.logical_or(d > 0, core != h)

                @pl.when(away)
                def _():
                    landed(kv.at[r, 0, d, h], KV, t).wait_send()

                @pl.when(jnp.logical_and(away, leaves(d, chip)))
                def _():
                    landed(q_in.at[slot], ROWS, t).wait_send()
                    landed(o_ref.at[seq(r, c)], OUT, t).wait_recv()
                    landed((dk_ref, dv_ref)[h].at[seq(r, c)], FIN, t).wait_recv()

                @pl.when(jnp.logical_and(away, leaves(d, wrap(chip - sign(r) * d))))
                def _():
                    landed(o_st.at[slot], OUT, t).wait_send()
                    landed(fin.at[slot, h], FIN, t).wait_send()

            @pl.when(stays(d, wrap(chip - sign(r) * d)))
            def _():
                home_cross(r).wait_send()

        return 0

    lax.fori_loop(0, n_far, drain, 0)
    for r in range(2):
        part_copy(r).wait_send()
    for h in range(2):
        @pl.when(core == h)
        def _():
            for r in range(2):
                for cp in own_out(r, h):
                    cp.wait()


def copy_kernel(*refs):
    n = (len(refs) - 2) // 3
    src, dst, buf, sem_in, sem_out = refs[:n], refs[n:2 * n], refs[2 * n:3 * n], refs[-2], refs[-1]
    ins = [pltpu.make_async_copy(src[a], buf[a], sem_in.at[a]) for a in range(n)]
    outs = [pltpu.make_async_copy(buf[a], dst[a], sem_out.at[a]) for a in range(n)]
    for cp in ins:
        cp.start()
    for cp_in, cp_out in zip(ins, outs):
        cp_in.wait()
        cp_out.start()
    for cp in outs:
        cp.wait()


def settle(*arrays):
    hbm = pl.BlockSpec(memory_space=pl.ANY)
    n = len(arrays)
    sems = pltpu.SemaphoreType.DMA((n,))
    return pl.pallas_call(
        copy_kernel,
        out_shape=tuple(jax.ShapeDtypeStruct(a.shape, a.dtype) for a in arrays),
        in_specs=[hbm] * n,
        out_specs=(hbm,) * n,
        scratch_shapes=[pltpu.VMEM(a.shape, a.dtype) for a in arrays] + [sems, sems],
    )(*arrays)


def solution(mesh):
    part_spec = P("dp", "ctx")
    n_ctx = mesh.shape["ctx"]
    n_chip = n_ctx // 2
    n_far = n_chip // 2

    def local_step(queries, keys, values, grad_out):
        n_batch, c_len, n_q, d_head = queries.shape
        assert keys.shape[2] == 1 and n_batch == n_chip
        rows = c_len * n_q // 2
        q_shape = (n_batch, 2, rows, d_head)
        kv_shape = (n_batch, c_len, d_head)
        hbm = pl.BlockSpec(memory_space=pl.ANY)
        vmem = pltpu.VMEM
        tiles = vmem((2 * n_far, 2, rows, d_head), BF16)
        out, grad_q, grad_k, grad_v = pl.pallas_call(
            functools.partial(kernel, n_chip, n_q, d_head ** -0.5),
            out_shape=tuple(jax.ShapeDtypeStruct(s, BF16) for s in (q_shape, q_shape, kv_shape, kv_shape)),
            in_specs=[hbm] * 4,
            out_specs=(hbm,) * 4,
            scratch_shapes=[
                tiles,
                tiles,
                vmem((2, 2, n_chip, 2, c_len, d_head), BF16),
                vmem((2, n_chip, d_head, 2 * c_len), BF16),
                vmem((2, n_chip, d_head, 2 * c_len), BF16),
                vmem((2, 2, n_chip, 2 * c_len, d_head), F32),
                vmem((2, n_chip, 2 * c_len, d_head), F32),
                vmem((2, n_far, 2 * c_len, d_head), F32),
                tiles,
                tiles,
                vmem((2 * n_far, 2, c_len, d_head), BF16),
                vmem((n_chip, 2 * c_len, 2 * rows), F32),
                vmem((d_head, 2 * rows), F32),
                vmem((d_head, 2 * rows), F32),
                vmem((2, 2, rows, d_head), BF16),
                vmem((2, 2, rows, d_head), BF16),
                vmem((2, 2, 2, c_len, d_head), BF16),
                vmem((2, 2, rows, d_head), BF16),
                vmem((2, 2, rows, d_head), BF16),
                vmem((2, 2, 2 * c_len, d_head), F32),
                vmem((2, 2 * c_len, d_head), F32),
                vmem((2, 2 * c_len, d_head), F32),
                vmem((2, 2, c_len, d_head), BF16),
                pltpu.SemaphoreType.DMA((N_KIND, n_ctx)),
                pltpu.SemaphoreType.DMA((N_KIND, n_ctx)),
                pltpu.SemaphoreType.DMA((N_SELF, 2)),
                pltpu.SemaphoreType.DMA((16,)),
            ],
            compiler_params=pltpu.CompilerParams(collective_id=0, has_side_effects=True, vmem_limit_bytes=62 * 2 ** 20),
        )(queries.reshape(q_shape), grad_out.reshape(q_shape), keys.reshape(kv_shape), values.reshape(kv_shape))
        out, grad_q, grad_k, grad_v = settle(out, grad_q, grad_k, grad_v)
        return (out.reshape(queries.shape), grad_q.reshape(queries.shape), grad_k.reshape(keys.shape), grad_v.reshape(values.shape))

    return jax.shard_map(local_step, mesh=mesh, in_specs=(part_spec,) * 4, out_specs=(part_spec,) * 4, check_vma=False)
```
